32 devices in a mesh: row: 4 (over y, core), col: 4 (over z), layer: 2 (over x).
Axes of the slice: x: 2, y: 2, z: 4, core: 2. Of those that a mesh axis runs over, the one named last changes fastest.
Arguments:
- a_tiles: float32 [16, 2, 7, 128, 128], P(('row', 'col'), 'layer'), may hold values from -0.5 to 0.5
- a_cols: int32 [16, 2, 7], P(('row', 'col'), 'layer'), may hold values from -1 to 255, as said below
- b_tiles: float32 [256, 2, 7, 128, 128], P(('row', 'col'), 'layer'), may hold values from -6 to 6
- b_rows: int32 [256, 2, 7], P(('row', 'col'), 'layer'), may hold values from 0 to 255, as said below
- c_cols: int32 [16, 4, 4], P('row', 'col'), may hold values from 0 to 255, as said below
Outputs:
- c_tiles: float32 [16, 4, 4, 128, 128], P('row', 'col', 'layer')
The draws below stay inside these ranges and needn't reach their ends.
Inputs may be any that keep to these rules, and one draw needn't show every extreme that they name: In a_cols[i, h, :] the used slots come first and hold distinct block columns in [h * 128, (h + 1) * 128); the unused ones hold -1. Some block rows use all 7 slots in each half, others few. b_rows[j, h, :] holds 7 distinct block rows in [h * 128, (h + 1) * 128). c_cols[i, g, :] holds 4 distinct block columns j with (j // 16) % 4 == g.
All inputs are finite; a program needn't handle non-finite values.
Results may differ from the reference program's by a relative error of at most 0.0003.
Values sent between devices are 32-bit elements; how exact they have to be, the bound alone decides.
No kernel may reach another device: no remote copies, remote signals or barrier semaphores. Data moves between devices by JAX's collectives and lax.ppermute only.
A program may use at most 128 MiB of HBM per device.

```python
import jax
import jax.numpy as jnp
from jax import lax

TILE = 128
NBLK = 256
RAH = 7
RBH = 7
RCC = 4
MROWS = 16
N_ROW = 4
N_COL = 4
N_LAYER = 2


def row_clusters(key):
    return jax.random.randint(jax.random.fold_in(key, 91), (MROWS,), 0, 4).astype(jnp.int32)


def draw_a_cols(key, part):
    half_count = NBLK // N_LAYER
    quarter = half_count // 4
    window = min(quarter, 2 * max(RAH, RBH))
    clusters = row_clusters(key)

    def one_slot(index):
        sub_key = jax.random.fold_in(key, index)
        layer_id = index % N_LAYER
        row_id = index // N_LAYER
        start = clusters[row_id] * quarter + layer_id * half_count
        picks = jax.random.permutation(sub_key, window)[:RAH].astype(jnp.int32) + start
        heavy = (jax.random.randint(jax.random.fold_in(sub_key, 7), (), 0, 4) == 0) | (row_id == 0)
        light = jax.random.randint(jax.random.fold_in(sub_key, 11), (), 1, RAH // 2 + 1)
        live = jnp.where(heavy, RAH, light)
        slots = jnp.arange(RAH, dtype=jnp.int32)
        return jnp.where(slots < live, picks, -1).astype(jnp.int32)
    values = jax.vmap(one_slot)(jnp.arange(MROWS * N_LAYER, dtype=jnp.int32))
    return values.reshape(MROWS, N_LAYER, RAH)


def draw_b_rows(key, part):
    half_count = NBLK // N_LAYER
    quarter = half_count // 4
    window = min(quarter, 2 * max(RAH, RBH))
    block_width = NBLK // (N_ROW * N_COL)

    def one_slot(index):
        sub_key = jax.random.fold_in(key, index + 3)
        column = index // N_LAYER
        layer_id = index % N_LAYER
        local = column // block_width // N_COL * block_width + column % block_width
        start = local % 4 * quarter + layer_id * half_count
        picks = jax.random.permutation(sub_key, window)[:RBH].astype(jnp.int32)
        return picks + start
    values = jax.vmap(one_slot)(jnp.arange(NBLK * N_LAYER, dtype=jnp.int32))
    return values.reshape(NBLK, N_LAYER, RBH).astype(jnp.int32)


def draw_c_cols(key, part):
    block_width = NBLK // (N_ROW * N_COL)
    per_cluster = NBLK // N_COL // 4
    clusters = row_clusters(key)

    def one_slot(index):
        sub_key = jax.random.fold_in(key, index + 5)
        row_id = index // N_COL
        group = index % N_COL
        local = jax.random.permutation(sub_key, per_cluster)[:RCC].astype(jnp.int32) * 4 + clusters[row_id]
        return (local // block_width * N_COL + group) * block_width + local % block_width
    values = jax.vmap(one_slot)(jnp.arange(MROWS * N_COL, dtype=jnp.int32))
    return values.reshape(MROWS, N_COL, RCC).astype(jnp.int32)


def block_scale(rng, shape, shards, smallest, high):
    factor_of, own = 1.0, jax.random.fold_in(rng, 6)
    for dim, shards_of in shards:
        heights = jnp.exp(jax.random.uniform(jax.random.fold_in(own, dim), (shards_of,), jnp.float32, smallest / len(shards), high / len(shards)))
        factor_of = factor_of * jnp.repeat(heights, shape[dim] // shards_of).reshape([-1 if axis == dim else 1 for axis in range(len(shape))])
    return factor_of


def bell_draw(stream_key, extent, scale, limit, pieces=(), kind=jnp.bfloat16):
    result = scale * jax.random.normal(stream_key, extent, jnp.float32)
    if pieces:
        result = result * block_scale(stream_key, extent, pieces, -0.22, 0.18)
    return jnp.clip(result, -limit, limit).astype(kind)


def setup_inputs(seed: int = 0) -> dict:
    splits = jax.random.split(jax.random.key(seed), 6)
    a_tiles = bell_draw(splits[0], (MROWS, N_LAYER, RAH, TILE, TILE), TILE ** -0.5, 0.5, ((0, 16), (1, 2)), jnp.float32)
    a_cols = draw_a_cols(jax.random.fold_in(splits[5], 71), 0)
    b_tiles = bell_draw(splits[2], (NBLK, N_LAYER, RBH, TILE, TILE), 1.0, 6.0, ((0, 16), (1, 2)), jnp.float32)
    b_rows = draw_b_rows(jax.random.fold_in(splits[5], 71), 0)
    c_cols = draw_c_cols(jax.random.fold_in(splits[5], 71), 0)
    return dict(a_tiles=a_tiles, a_cols=a_cols, b_tiles=b_tiles, b_rows=b_rows, c_cols=c_cols)


def reference(a_tiles, a_cols, b_tiles, b_rows, c_cols):
    halves = b_rows.shape[1]
    slot_count = b_rows.shape[2]
    b_flat = b_tiles.reshape((-1,) + b_tiles.shape[3:])

    def one_row(inputs):
        a_row, a_index, wanted = inputs
        columns = wanted.reshape(-1).astype(jnp.int32)
        col_rows = b_rows[columns]
        matches = (col_rows[:, :, None, :] == a_index[None, :, :, None]) & (a_index >= 0)[None, :, :, None]
        present = jnp.any(matches, axis=3)
        position = jnp.argmax(matches, axis=3).astype(jnp.int32)
        layer_ids = jnp.arange(halves, dtype=jnp.int32)
        flat_index = (columns[:, None, None] * halves + layer_ids[None, :, None]) * slot_count + position
        chosen = jnp.take(b_flat, flat_index.reshape(-1), axis=0)
        chosen = chosen.reshape(flat_index.shape + b_flat.shape[1:])
        chosen = jnp.where(present[..., None, None], chosen, jnp.zeros((), chosen.dtype))
        product = jnp.einsum("heab,qhebc->qac", a_row, chosen, precision=lax.Precision.HIGHEST)
        return product.reshape(wanted.shape + product.shape[1:])

    return lax.map(one_row, (a_tiles, a_cols, c_cols))
```

```python
import functools

import jax
import jax.numpy as jnp
import numpy as np
from jax import lax
from jax.experimental import pallas as pl
from jax.experimental.pallas import tpu as pltpu
from jax.sharding import PartitionSpec as P

AXES = ("row", "col", "layer")
SMEM = pltpu.SMEM
VMEM = pltpu.VMEM
ANY = pl.ANY
I32 = jnp.int32


def plan_kernel(dims, me, gs, gv, jcol, jlay, out_ref, in_ref, lvl_ref, need):
    R, G, L, W, S, AR, SA, RPD, Q, PAIR, Y, NB, caps = dims
    GL = G * L
    b = gv[:, :NB]
    col_of = jcol[...]
    lay_of = jlay[...]
    most = jnp.int32(0)
    for d in range(Y):

        def one_row(i, acc):
            r = d * PAIR + i // RPD
            ci = i % RPD
            wanted = None
            for g in range(G):
                for q in range(Q):
                    hit = col_of == gs[(r * G + g) * L, NB + AR * SA + ci * Q + q]
                    wanted = hit if wanted is None else wanted | hit
            match = None
            for s in range(SA):
                want = jnp.full(b.shape, gs[(r * G + ci // AR) * L, NB + (ci % AR) * SA + s], I32)
                for l in range(1, L):
                    want = jnp.where(
                        lay_of == l, gs[(r * G + ci // AR) * L + l, NB + (ci % AR) * SA + s], want
                    )
                hit = b == want
                match = hit if match is None else match | hit
            return jnp.where(wanted & match, 1, acc)

        acc = lax.fori_loop(0, PAIR * RPD, one_row, jnp.zeros(b.shape, I32))
        need[d] = acc
        per_dev = jnp.sum(acc.astype(jnp.float32).reshape(Y, PAIR, GL, NB), axis=1)
        per_chip = jnp.sum(per_dev, axis=2)
        chip = lax.broadcasted_iota(I32, per_chip.shape, 0)
        most = jnp.maximum(most, jnp.max(jnp.where(chip == d, 0.0, per_chip)).astype(I32))
    share = (most + PAIR - 1) // PAIR
    level = jnp.int32(0)
    for cap in caps[:-1]:
        level = level + (share > cap).astype(I32)
    lvl_ref[0] = level
    y = me[0] // PAIR
    mine = me[1] * L + me[2]
    for delta in range(1, Y):
        dst = (y + delta) % Y
        src = (y + Y - delta) % Y
        for c in range(PAIR):
            out_ref[delta - 1, c : c + 1, :] = need[dst, pl.ds((y * PAIR + c) * GL + mine, 1), :]
            in_ref[delta - 1, c : c + 1, :] = need[y, pl.ds((src * PAIR + c) * GL + mine, 1), :]


def pack_kernel(dims, me, bits, own, sib, out, sem):
    R, G, L, W, S, AR, SA, RPD, Q, PAIR, Y, NB, caps = dims
    core = me[0] % PAIR
    total = jnp.int32(0)
    for delta in range(Y - 1):
        p = jnp.int32(0)
        for c in range(PAIR):

            def one(t, p):
                take = (bits[delta, c, t] != 0) & (p % PAIR == core)
                dst = out.at[delta, p // PAIR]

                @pl.when(take & (core == c))
                def _():
                    pltpu.make_async_copy(own.at[t], dst, sem).start()

                @pl.when(take & (core != c))
                def _():
                    pltpu.make_async_copy(sib.at[t], dst, sem).start()

                return p + bits[delta, c, t]

            p = lax.fori_loop(0, NB, one, p)
        total = total + (p - core + PAIR - 1) // PAIR

    def wait(k, _):
        pltpu.make_async_copy(own.at[0], out.at[0, 0], sem).wait()
        return 0

    lax.fori_loop(0, total, wait, 0)


def list_kernel(dims, me, gs, bits, src_ref, aidx_ref, oidx_ref, starts_ref, pos):
    R, G, L, W, S, AR, SA, RPD, Q, PAIR, Y, NB, caps = dims
    QL = Q // L
    row, col, lay = me[0], me[1], me[2]
    y = row // PAIR
    for delta in range(Y - 1):
        p = jnp.int32(0)
        for c in range(PAIR):

            def scan(t, p):
                pos[delta, c * NB + t] = p
                return p + bits[delta, c, t]

            p = lax.fori_loop(0, NB, scan, p)
    n = jnp.int32(0)
    for k in range(L):
        step = (k + 1) % L
        starts_ref[k] = n
        half = (lay + step) % L

        def one_pair(i, n):
            ci = i // QL
            qq = i % QL
            j = gs[(row * G + col) * L + lay, NB + AR * SA + ci * Q + half * QL + qq]
            rp = j // (G * W)
            w = j % W
            chip = rp // PAIR
            a_dev = (row * G + ci // AR) * L + lay
            a_vals = [gs[a_dev, NB + (ci % AR) * SA + s] for s in range(SA)]
            a_base = ((col + G - ci // AR) % G) * AR * SA + (ci % AR) * SA
            delta = (y + Y - chip) % Y

            def one_slot(sl, n):
                b = gs[(rp * G + col) * L + lay, w * S + sl]
                s_hit = jnp.int32(-1)
                for s in range(SA):
                    s_hit = jnp.where(b == a_vals[s], s, s_hit)
                tile = w * S + sl
                here = jnp.where(rp == row, tile, NB + tile)
                there = pos[jnp.maximum(delta - 1, 0), (rp % PAIR) * NB + tile]
                src = jnp.where(delta == 0, here, 2 * NB * (delta + 0) + there)
                src_ref[n] = src
                aidx_ref[n] = a_base + jnp.maximum(s_hit, 0)
                oidx_ref[n] = i
                return n + (s_hit >= 0).astype(I32)

            return lax.fori_loop(0, S, one_slot, n)

        n = lax.fori_loop(0, RPD * QL, one_pair, n)
    starts_ref[L] = n


def select_kernel(dims, me, src, starts, own, sib, rec, rec2, out, sem):
    R, G, L, W, S, AR, SA, RPD, Q, PAIR, Y, NB, caps = dims
    core = me[0] % PAIR
    n = starts[L]

    def one(k, _):
        s = src[k]
        dst = out.at[k]

        @pl.when(s < NB)
        def _():
            pltpu.make_async_copy(own.at[jnp.minimum(s, NB - 1)], dst, sem).start()

        @pl.when((s >= NB) & (s < 2 * NB))
        def _():
            pltpu.make_async_copy(sib.at[jnp.clip(s - NB, 0, NB - 1)], dst, sem).start()

        @pl.when(s >= 2 * NB)
        def _():
            rest = s - 2 * NB
            delta = rest // (2 * NB)
            p = rest % (2 * NB)

            @pl.when(p % PAIR == core)
            def _():
                pltpu.make_async_copy(rec.at[delta, p // PAIR], dst, sem).start()

            @pl.when(p % PAIR != core)
            def _():
                pltpu.make_async_copy(rec2.at[delta, p // PAIR], dst, sem).start()

        return 0

    lax.fori_loop(0, n, one, 0)

    def wait(k, _):
        pltpu.make_async_copy(own.at[0], out.at[0], sem).wait()
        return 0

    lax.fori_loop(0, n, wait, 0)


def product_kernel(dims, chunk, depth, aidx, oidx, starts, sel, *refs):
    R, G, L, W, S, AR, SA, RPD, Q, PAIR, Y, NB, caps = dims
    a_refs, out, a_all, buf, a_sem, b_sem = refs[:G], refs[G], *refs[G + 1 :]
    first, last = starts[chunk], starts[chunk + 1]
    n = last - first

    def fetch(k):
        return pltpu.make_async_copy(sel.at[first + k], buf.at[k % depth], b_sem.at[k % depth])

    for k in range(G):
        pltpu.make_async_copy(a_refs[k], a_all.at[pl.ds(k * AR * SA, AR * SA)], a_sem.at[k]).start()
    for k in range(depth):

        @pl.when(k < n)
        def _():
            fetch(k).start()

    out[...] = jnp.zeros(out.shape, out.dtype)
    for k in range(G):
        pltpu.make_async_copy(a_refs[k], a_all.at[pl.ds(k * AR * SA, AR * SA)], a_sem.at[k]).wait()

    def one(k, _):
        fetch(k).wait()
        a = a_all[aidx[first + k]]
        b = buf[k % depth]
        a_hi = a.astype(jnp.bfloat16)
        b_hi = b.astype(jnp.bfloat16)
        a_lo = (a - a_hi.astype(jnp.float32)).astype(jnp.bfloat16)
        b_lo = (b - b_hi.astype(jnp.float32)).astype(jnp.bfloat16)
        dot = functools.partial(jnp.dot, preferred_element_type=jnp.float32)
        o = oidx[first + k]
        out[o] = out[o] + (dot(a_hi, b_hi) + (dot(a_hi, b_lo) + dot(a_lo, b_hi)))

        @pl.when(k + depth < n)
        def _():
            fetch(k + depth).start()

        return 0

    lax.fori_loop(0, n, one, 0)


def on_device(a_tiles, a_cols, b_tiles, b_rows, c_cols):
    R, G, L = (lax.axis_size(name) for name in AXES)
    W, S, T = b_tiles.shape[0], b_tiles.shape[2], b_tiles.shape[-1]
    AR, SA = a_tiles.shape[0], a_tiles.shape[2]
    RPD, Q = c_cols.shape[0], c_cols.shape[2]
    PAIR = 2 if R % 2 == 0 else 1
    Y, NB, N, QL = R // PAIR, W * S, R * G * L, Q // L
    full = -(-PAIR * NB // PAIR)
    caps = tuple(sorted({-(-full * k // 28) for k in (4, 5, 6, 7, 8, 11, 16, 28)}))
    dims = (R, G, L, W, S, AR, SA, RPD, Q, PAIR, Y, NB, caps)
    f32 = jnp.float32
    smem = pl.BlockSpec(memory_space=SMEM)
    vmem = pl.BlockSpec(memory_space=VMEM)
    hbm = pl.BlockSpec(memory_space=ANY)

    own = b_tiles.reshape(NB, T, T)
    pair_swap = [(r, r ^ 1) for r in range(R)] if PAIR == 2 else [(r, r) for r in range(R)]
    sib = lax.ppermute(own, "row", pair_swap)
    a_own = a_tiles.reshape(AR * SA, T, T)
    a_list = [a_own] + [
        lax.ppermute(a_own, "col", [(c, (c + d) % G) for c in range(G)]) for d in range(1, G)
    ]
    me = jnp.stack([lax.axis_index(name) for name in AXES]).astype(I32)
    idx = jnp.concatenate([b_rows.reshape(-1), a_cols.reshape(-1), c_cols.reshape(-1)])
    table = lax.all_to_all(jnp.broadcast_to(idx[None], (N,) + idx.shape), AXES, 0, 0, tiled=True)

    blocks = np.arange(N)[:, None] // L
    jcol = (blocks * W + np.arange(NB)[None] // S).astype(np.int32)
    jlay = np.broadcast_to(np.arange(N)[:, None] % L, (N, NB)).astype(np.int32)
    bits_shape = jax.ShapeDtypeStruct((max(Y - 1, 1), PAIR, NB), I32)
    out_bits, in_bits, level = pl.pallas_call(
        functools.partial(plan_kernel, dims),
        in_specs=[smem, smem, vmem, vmem, vmem],
        out_specs=[vmem, vmem, smem],
        out_shape=[bits_shape, bits_shape, jax.ShapeDtypeStruct((1,), I32)],
        scratch_shapes=[VMEM((Y, N, NB), I32)],
        name="plan",
    )(me, table, table, jnp.asarray(jcol), jnp.asarray(jlay))

    most = RPD * Q * S

    def fetch(cap, me, table, out_bits, in_bits, own, sib):
        packed = pl.pallas_call(
            functools.partial(pack_kernel, dims),
            in_specs=[smem, smem, hbm, hbm],
            out_specs=hbm,
            out_shape=jax.ShapeDtypeStruct((max(Y - 1, 1), cap, T, T), f32),
            scratch_shapes=[pltpu.SemaphoreType.DMA],
            name="pack",
        )(me, out_bits, own, sib)
        recs = [
            lax.ppermute(
                packed[delta - 1 : delta],
                "row",
                [(r, ((r // PAIR + delta) % Y) * PAIR + r % PAIR) for r in range(R)],
            )
            for delta in range(1, Y)
        ]
        rec = recs[0] if len(recs) == 1 else jnp.concatenate(recs, 0)
        rec2 = lax.ppermute(rec, "row", pair_swap)
        src, aidx, oidx, starts = pl.pallas_call(
            functools.partial(list_kernel, dims),
            in_specs=[smem, smem, smem],
            out_specs=[smem, smem, smem, smem],
            out_shape=[jax.ShapeDtypeStruct((most + 1,), I32)] * 3
            + [jax.ShapeDtypeStruct((L + 1,), I32)],
            scratch_shapes=[SMEM((max(Y - 1, 1), PAIR * NB), I32)],
            cost_estimate=pl.CostEstimate(flops=10**8, bytes_accessed=10**5, transcendentals=0),
            name="list",
        )(me, table, in_bits)
        sel = pl.pallas_call(
            functools.partial(select_kernel, dims),
            in_specs=[smem, smem, smem, hbm, hbm, hbm, hbm],
            out_specs=hbm,
            out_shape=jax.ShapeDtypeStruct((most, T, T), f32),
            scratch_shapes=[pltpu.SemaphoreType.DMA],
            name="select",
        )(me, src, starts, own, sib, rec, rec2)
        return sel, aidx, oidx, starts

    sel, aidx, oidx, starts = lax.switch(
        level[0],
        [functools.partial(fetch, cap) for cap in caps],
        me, table, out_bits, in_bits, own, sib,
    )
    depth = 8

    def products(chunk):
        return pl.pallas_call(
            functools.partial(product_kernel, dims, chunk, depth),
            in_specs=[smem, smem, smem, hbm] + [hbm] * G,
            out_specs=vmem,
            out_shape=jax.ShapeDtypeStruct((RPD * QL, T, T), f32),
            scratch_shapes=[
                VMEM((G * AR * SA, T, T), f32),
                VMEM((depth, T, T), f32),
                pltpu.SemaphoreType.DMA((G,)),
                pltpu.SemaphoreType.DMA((depth,)),
            ],
            cost_estimate=pl.CostEstimate(flops=2 * 10**9, bytes_accessed=10**6, transcendentals=0),
            name="products",
        )(aidx, oidx, starts, sel, *a_list)

    moved = [
        lax.ppermute(products(k), "layer", [(l, (l + k + 1) % L) for l in range(L)])
        for k in range(L - 1)
    ]
    result = products(L - 1)
    for part in moved:
        result = result + part
    return result.reshape(RPD, 1, QL, T, T)


def solution(mesh):
    return jax.shard_map(
        on_device,
        mesh=mesh,
        in_specs=(
            P(("row", "col"), "layer", None, None, None),
            P(("row", "col"), "layer", None),
            P(("row", "col"), "layer", None, None, None),
            P(("row", "col"), "layer", None),
            P("row", "col", None),
        ),
        out_specs=P("row", "col", "layer", None, None),
        check_vma=False,
    )
```

```python
import functools

import jax
import jax.numpy as jnp
import numpy as np
from jax import lax
from jax.experimental import pallas as pl
from jax.experimental.pallas import tpu as pltpu
from jax.sharding import PartitionSpec as P

AXES = ("row", "col", "layer")
SMEM = pltpu.SMEM
VMEM = pltpu.VMEM
HBM = pltpu.HBM
I32 = jnp.int32
F32 = jnp.float32
BF16 = jnp.bfloat16


def plan_kernel(d, me, gs, gv, jcol, jlay, tri, inv_ref, cnt_ref, pos_ref, lvl_ref, need, need_send):
    b = gv[:, : d.NB]
    col_of = jcol[...]
    lay_of = jlay[...]
    most, most_send = jnp.int32(0), jnp.int32(0)

    def per_chip(x):
        return jnp.sum(jnp.sum(x.astype(F32).reshape(d.Y, d.PAIR, d.G * d.L, d.NB), axis=1), axis=2)

    for dst in range(d.Y):

        def one_row(i, acc):
            r = dst * d.PAIR + i // d.RPD
            ci = i % d.RPD
            wanted, wanted_send = None, None
            for h in range(d.L):
                part = None
                for g in range(d.G):
                    for q in range(h * d.QL, (h + 1) * d.QL):
                        hit = col_of == gs[(r * d.G + g) * d.L, d.OFF_C + ci * d.Q + q]
                        part = hit if part is None else part | hit
                away = part & (lay_of != h)
                wanted = part if wanted is None else wanted | part
                wanted_send = away if wanted_send is None else wanted_send | away
            match = None
            base = (r * d.G + ci // d.AR) * d.L
            for s in range(d.SA):
                at = d.NB + (ci % d.AR) * d.SA + s
                want = jnp.full(b.shape, gs[base, at], I32)
                for l in range(1, d.L):
                    want = jnp.where(lay_of == l, gs[base + l, at], want)
                hit = b == want
                match = hit if match is None else match | hit
            return (
                jnp.where(wanted & match, 1, acc[0]),
                jnp.where(wanted_send & match, 1, acc[1]),
            )

        zero = jnp.zeros(b.shape, I32)
        acc, send = lax.fori_loop(0, d.PAIR * d.RPD, one_row, (zero, zero))
        need[dst] = acc
        need_send[dst] = send
        chip = lax.broadcasted_iota(I32, (d.Y, d.G * d.L), 0)
        away = chip != dst
        most = jnp.maximum(most, jnp.max(jnp.where(away, per_chip(acc), 0.0)).astype(I32))
        most_send = jnp.maximum(most_send, jnp.max(jnp.where(away, per_chip(send), 0.0)).astype(I32))
    share = (most + d.PAIR - 1) // d.PAIR
    share_send = (most_send + d.PAIR - 1) // d.PAIR
    level = jnp.int32(0)
    for first, cap in d.caps[:-1]:
        level = level + ((share > cap) | (share_send > first)).astype(I32)
    lvl_ref[0] = level

    y = me[0] // d.PAIR
    mine = me[1] * d.L + me[2]
    lanes = lax.broadcasted_iota(I32, (d.NB, d.PAIR * d.NB), 1).astype(F32)
    ones = jnp.ones((8, d.NB), F32)

    def rows_of(ref, dst, src, c):
        return ref[dst, pl.ds((src * d.PAIR + c) * d.G * d.L + mine, 1), :].astype(F32)

    for delta in range(1, d.Y):
        dst = (y + delta) % d.Y
        src = (y + d.Y - delta) % d.Y
        for kind in range(2):
            before = jnp.float32(0)
            inv = jnp.zeros((1, d.PAIR * d.NB), F32)
            for c in range(d.PAIR):
                bits = rows_of(need_send, dst, y, c)
                if kind == 1:
                    bits = rows_of(need, dst, y, c) - bits
                wide = ones * bits
                upto = lax.dot_general(tri[...], wide, (((0,), (1,)), ((), ())), preferred_element_type=F32)
                inv = inv + jnp.sum(
                    jnp.where(upto[:, :1] + before <= lanes, 1.0, 0.0), axis=0, keepdims=True
                )
                before = before + jnp.sum(bits)
            inv_ref[delta - 1, kind : kind + 1, :] = inv.astype(I32)
            cnt_ref[delta - 1, kind] = before.astype(I32)
        before = jnp.float32(0)
        position = [None] * d.PAIR
        for kind in range(2):
            for c in range(d.PAIR):
                bits = rows_of(need_send, y, src, c)
                if kind == 1:
                    bits = rows_of(need, y, src, c) - bits
                ahead = jnp.dot(ones * bits, tri[...], preferred_element_type=F32)[:1] - bits + before
                position[c] = ahead if kind == 0 else jnp.where(bits > 0.5, ahead, position[c])
                before = before + jnp.sum(bits)
        for c in range(d.PAIR):
            pos_ref[delta - 1, c : c + 1, :] = position[c].astype(I32)


def pack_kernel(d, first, cap, me, inv, cnt, own, sib, out, out2, sem):
    core = me[0] % d.PAIR
    total = jnp.int32(0)
    for delta in range(d.Y - 1):
        send = cnt[delta, 0]
        count = (send + cnt[delta, 1] - core + d.PAIR - 1) // d.PAIR

        def one(k, _):
            p = k * d.PAIR + core
            late = jnp.maximum(p - send, 0)
            t = jnp.where(p < send, inv[delta, 0, p], inv[delta, 1, late])
            c = t // d.NB
            t = t % d.NB

            def put(dst):
                @pl.when(c == core)
                def _():
                    pltpu.make_async_copy(own.at[t], dst, sem).start()

                @pl.when(c != core)
                def _():
                    pltpu.make_async_copy(sib.at[t], dst, sem).start()

            @pl.when(k < first)
            def _():
                put(out.at[delta, jnp.minimum(k, first - 1)])

            if cap > first:

                @pl.when(k >= first)
                def _():
                    put(out2.at[delta, jnp.clip(k - first, 0, cap - first - 1)])

            return 0

        lax.fori_loop(0, count, one, 0)
        total = total + count

    def wait(k, _):
        pltpu.make_async_copy(own.at[0], out.at[0, 0], sem).wait()
        return 0

    lax.fori_loop(0, total, wait, 0)


def list_kernel(d, me, gs, pos, src_ref, aidx_ref, oidx_ref, starts_ref):
    row, col, lay = me[0], me[1], me[2]
    y = row // d.PAIR
    n = jnp.int32(0)
    for k, (step, low, high) in enumerate(d.sections):
        starts_ref[k] = n
        half = (lay + step) % d.L

        def one_pair(i, n):
            sl_d = i // (d.AR * d.QL)
            ar = i // d.QL % d.AR
            qq = i % d.QL
            cc = (col + d.G - (low + sl_d)) % d.G
            ci = cc * d.AR + ar
            j = gs[(row * d.G + col) * d.L + lay, d.OFF_C + ci * d.Q + half * d.QL + qq]
            rp = j // (d.G * d.W)
            w = j % d.W
            a_dev = (row * d.G + cc) * d.L + lay
            a_vals = [gs[a_dev, d.NB + ar * d.SA + s] for s in range(d.SA)]
            a_base = (sl_d * d.AR + ar) * d.SA
            delta = (y + d.Y - rp // d.PAIR) % d.Y
            here = jnp.where(rp == row, 0, d.NB)

            def one_slot(sl, n):
                tile = w * d.S + sl
                b = gs[(rp * d.G + col) * d.L + lay, tile]
                s_hit = jnp.int32(-1)
                for s in range(d.SA):
                    s_hit = jnp.where(b == a_vals[s], s, s_hit)

                @pl.when(s_hit >= 0)
                def _():
                    there = pos[jnp.maximum(delta - 1, 0), rp % d.PAIR, tile]
                    src_ref[n] = jnp.where(delta == 0, here + tile, 2 * d.NB * delta + there)
                    aidx_ref[n] = a_base + s_hit
                    oidx_ref[n] = i

                return n + (s_hit >= 0).astype(I32)

            return lax.fori_loop(0, d.S, one_slot, n)

        n = lax.fori_loop(0, (high - low) * d.AR * d.QL, one_pair, n)
    starts_ref[len(d.sections)] = n


def product_kernel(d, section, depth, first_cap, n_a, two, me, src, aidx, oidx, starts, *refs):
    n_b = 6 if two else 4
    b_refs, a_refs, out = refs[:n_b], refs[n_b : n_b + n_a], refs[n_b + n_a]
    a_all, buf, sem = refs[n_b + n_a + 1 :]
    core = me[0] % d.PAIR
    first = starts[section]
    n = starts[section + 1] - first

    def start(k):
        s = src[first + k]
        dst = buf.at[k % depth]
        done = sem.at[k % depth]

        @pl.when(s < d.NB)
        def _():
            pltpu.make_async_copy(b_refs[0].at[jnp.minimum(s, d.NB - 1)], dst, done).start()

        @pl.when((s >= d.NB) & (s < 2 * d.NB))
        def _():
            pltpu.make_async_copy(b_refs[1].at[jnp.clip(s - d.NB, 0, d.NB - 1)], dst, done).start()

        @pl.when(s >= 2 * d.NB)
        def _():
            rest = s - 2 * d.NB
            delta = rest // (2 * d.NB)
            p = rest % (2 * d.NB)
            slot = p // d.PAIR
            straight = p % d.PAIR == core
            for piece in range(2 if two else 1):
                at = slot - piece * first_cap
                inside = (slot < first_cap) if piece == 0 else (slot >= first_cap)
                at = jnp.clip(at, 0, b_refs[2 + 2 * piece].shape[1] - 1)

                @pl.when(inside & straight)
                def _():
                    pltpu.make_async_copy(b_refs[2 + 2 * piece].at[delta, at], dst, done).start()

                @pl.when(inside & jnp.logical_not(straight))
                def _():
                    pltpu.make_async_copy(b_refs[3 + 2 * piece].at[delta, at], dst, done).start()

    for k in range(depth):

        @pl.when(k < n)
        def _():
            start(jnp.int32(k))

    rows = d.AR * d.SA
    T = d.T
    for k in range(n_a):
        a = a_refs[k][...]
        hi = a.astype(BF16)
        a_all[k * rows : (k + 1) * rows, :T, :] = hi
        a_all[k * rows : (k + 1) * rows, T:, :] = (a - hi.astype(F32)).astype(BF16)
    out[...] = jnp.zeros(out.shape, out.dtype)

    def one(k, _):
        pltpu.make_async_copy(b_refs[0].at[0], buf.at[k % depth], sem.at[k % depth]).wait()
        b = buf[k % depth]
        b_hi = b.astype(BF16)
        b_lo = (b - b_hi.astype(F32)).astype(BF16)
        a = a_all[aidx[first + k]]
        both = jnp.dot(a, b_hi, preferred_element_type=F32)
        low = jnp.dot(a[:T], b_lo, preferred_element_type=F32)
        o = oidx[first + k]
        out[o] = out[o] + (both[:T] + (both[T:] + low))

        @pl.when(k + depth < n)
        def _():
            start(k + depth)

        return 0

    lax.fori_loop(0, n, one, 0)


def merge_kernel(d, me, *refs):
    own, out = refs[-2], refs[-1]
    col = me[1]
    size = d.AR * d.QL
    for k in range(d.G):
        part = own[k * size : (k + 1) * size]
        for m in range(d.L - 1):
            early, late = refs[2 * m], refs[2 * m + 1]
            part = part + (
                early[k * size : (k + 1) * size]
                if k < d.EARLY
                else late[(k - d.EARLY) * size : (k - d.EARLY + 1) * size]
            )
        out[pl.ds((col + d.G - k) % d.G * size, size)] = part


class Dims:
    pass


def on_device(a_tiles, a_cols, b_tiles, b_rows, c_cols):
    d = Dims()
    d.R, d.G, d.L = (lax.axis_size(name) for name in AXES)
    d.W, d.S, d.T = b_tiles.shape[0], b_tiles.shape[2], b_tiles.shape[-1]
    d.AR, d.SA = a_tiles.shape[0], a_tiles.shape[2]
    d.RPD, d.Q = c_cols.shape[0], c_cols.shape[2]
    d.PAIR = 2 if d.R % 2 == 0 else 1
    d.Y, d.NB, d.N, d.QL = d.R // d.PAIR, d.W * d.S, d.R * d.G * d.L, d.Q // d.L
    d.OFF_C = d.NB + d.AR * d.SA
    d.EARLY = 1 + max(1, d.G // 4)
    totals = sorted({-(-d.NB * k // 56) for k in (8, 9, 10, 11, 12, 14, 18, 28)})
    d.caps = tuple((-(-t * 5 // 8), t) for t in totals) + ((d.NB, d.NB),)
    d.sections = tuple(
        (step, low, high)
        for step in range(1, d.L)
        for low, high in ((0, d.EARLY), (d.EARLY, d.G))
    ) + ((0, 0, d.G),)
    R, G, L, T, NB, PAIR, Y = d.R, d.G, d.L, d.T, d.NB, d.PAIR, d.Y
    YS = max(Y - 1, 1)
    smem = pl.BlockSpec(memory_space=SMEM)
    vmem = pl.BlockSpec(memory_space=VMEM)
    hbm = pl.BlockSpec(memory_space=HBM)

    def shift(x, k):
        return lax.ppermute(x, "col", [(c, (c + k) % G) for c in range(G)])

    own = b_tiles.reshape(NB, T, T)
    pair_swap = [(r, r ^ (PAIR - 1)) for r in range(R)]
    a_own = a_tiles.reshape(d.AR * d.SA, T, T)
    me = jnp.stack([lax.axis_index(name) for name in AXES]).astype(I32)
    idx = jnp.concatenate([b_rows.reshape(-1), a_cols.reshape(-1), c_cols.reshape(-1)])
    n_idx = idx.shape[0]
    near = [idx] + [shift(idx, k) for k in range(1, G)]
    sib = lax.ppermute(own, "row", pair_swap)
    a_early = [a_own] + [shift(a_own, k) for k in range(1, d.EARLY)]
    group = jnp.stack(near)
    col = lax.axis_index("col")
    group = jnp.roll(group[::-1], col + 1, axis=0)
    table = lax.all_to_all(
        jnp.broadcast_to(group[None], (R * L, G, n_idx)), ("row", "layer"), 0, 0, tiled=True
    )
    table = table.reshape(R, L, G, n_idx).transpose(0, 2, 1, 3).reshape(d.N, n_idx)

    blocks = np.arange(d.N)[:, None] // L
    jcol = (blocks * d.W + np.arange(NB)[None] // d.S).astype(np.int32)
    jlay = np.broadcast_to(np.arange(d.N)[:, None] % L, (d.N, NB)).astype(np.int32)
    tri = np.triu(np.ones((NB, NB), np.float32))
    inv, cnt, pos, level = pl.pallas_call(
        functools.partial(plan_kernel, d),
        in_specs=[smem, smem, vmem, vmem, vmem, vmem],
        out_specs=[vmem, smem, vmem, smem],
        out_shape=[
            jax.ShapeDtypeStruct((YS, 2, PAIR * NB), I32),
            jax.ShapeDtypeStruct((YS, 2), I32),
            jax.ShapeDtypeStruct((YS, PAIR, NB), I32),
            jax.ShapeDtypeStruct((1,), I32),
        ],
        scratch_shapes=[VMEM((Y, d.N, NB), I32)] * 2,
        name="plan",
    )(me, table, table, jnp.asarray(jcol), jnp.asarray(jlay), jnp.asarray(tri))

    most = d.RPD * d.Q * d.S

    def run(caps, me, table, inv, cnt, pos, own, sib, *a_early):
        first, cap = caps
        second = max(cap - first, 1)
        packs = pl.pallas_call(
            functools.partial(pack_kernel, d, first, cap),
            in_specs=[smem, smem, smem, hbm, hbm],
            out_specs=[vmem, vmem],
            out_shape=[
                jax.ShapeDtypeStruct((YS, first, T, T), F32),
                jax.ShapeDtypeStruct((YS, second, T, T), F32),
            ],
            scratch_shapes=[pltpu.SemaphoreType.DMA],
            name="pack",
        )(me, inv, cnt, own, sib)
        two = cap > first

        def across(packed):
            recs = [
                lax.ppermute(
                    packed[k - 1 : k],
                    "row",
                    [(r, ((r // PAIR + k) % Y) * PAIR + r % PAIR) for r in range(R)],
                )
                for k in range(1, Y)
            ]
            rec = recs[0] if len(recs) == 1 else jnp.concatenate(recs, 0)
            return [rec, lax.ppermute(rec, "row", pair_swap)]

        received = [across(p) for p in packs[: 2 if two else 1]]
        a_late = [shift(a_early[0], k) for k in range(d.EARLY, G)]
        a_list = list(a_early) + a_late
        src, aidx, oidx, starts = pl.pallas_call(
            functools.partial(list_kernel, d),
            in_specs=[smem, smem, smem],
            out_specs=[smem, smem, smem, smem],
            out_shape=[jax.ShapeDtypeStruct((most,), I32)] * 3
            + [jax.ShapeDtypeStruct((len(d.sections) + 1,), I32)],
            cost_estimate=pl.CostEstimate(flops=5 * 10**9, bytes_accessed=10**5, transcendentals=0),
            name="list",
        )(me, table, pos)

        depth = 8

        def products(k):
            step, low, high = d.sections[k]
            with_second = two and step == 0
            b_list = [own, sib] + received[0] + (received[1] if with_second else [])
            a_part = a_list[low:high]
            return pl.pallas_call(
                functools.partial(product_kernel, d, k, depth, first, len(a_part), with_second),
                in_specs=[smem] * 5 + [hbm] * len(b_list) + [vmem] * len(a_part),
                out_specs=vmem,
                out_shape=jax.ShapeDtypeStruct(((high - low) * d.AR * d.QL, T, T), F32),
                scratch_shapes=[
                    VMEM((len(a_part) * d.AR * d.SA, 2 * T, T), BF16),
                    VMEM((depth, T, T), F32),
                    pltpu.SemaphoreType.DMA((depth,)),
                ],
                cost_estimate=pl.CostEstimate(
                    flops=5 * 10**9, bytes_accessed=10**6, transcendentals=0
                ),
                name="products",
            )(me, src, aidx, oidx, starts, *b_list, *a_part)

        moved = [
            lax.ppermute(products(k), "layer", [(l, (l + step) % L) for l in range(L)])
            for k, (step, _, _) in enumerate(d.sections[:-1])
        ]
        mine = products(len(d.sections) - 1)
        return pl.pallas_call(
            functools.partial(merge_kernel, d),
            in_specs=[smem] + [vmem] * (len(moved) + 1),
            out_specs=vmem,
            out_shape=jax.ShapeDtypeStruct((d.RPD * d.QL, T, T), F32),
            name="merge",
        )(me, *moved, mine)

    result = lax.switch(
        level[0],
        [functools.partial(run, caps) for caps in d.caps],
        me, table, inv, cnt, pos, own, sib, *a_early,
    )
    return result.reshape(d.RPD, 1, d.QL, T, T)


def solution(mesh):
    return jax.shard_map(
        on_device,
        mesh=mesh,
        in_specs=(
            P(("row", "col"), "layer", None, None, None),
            P(("row", "col"), "layer", None),
            P(("row", "col"), "layer", None, None, None),
            P(("row", "col"), "layer", None),
            P("row", "col", None),
        ),
        out_specs=P("row", "col", "layer", None, None),
        check_vma=False,
    )
```

```python
import functools

import jax
import jax.numpy as jnp
import numpy as np
from jax import lax
from jax.experimental import pallas as pl
from jax.experimental.pallas import tpu as pltpu
from jax.sharding import PartitionSpec as P


AXES = ("row", "col", "layer")
SMEM = pltpu.SMEM
VMEM = pltpu.VMEM
HBM = pltpu.HBM
I32 = jnp.int32
F32 = jnp.float32
BF16 = jnp.bfloat16


def index_kernel(d, b_rows, a_cols, c_cols, out):
    for w in range(d.W):
        for s in range(d.S):
            out[0, w * d.S + s] = b_rows[s, 0, w]
    for r in range(d.AR):
        for s in range(d.SA):
            out[0, d.NB + r * d.SA + s] = a_cols[r, 0, s]
    for r in range(d.RPD):
        for q in range(d.Q):
            out[0, d.OFF_C + r * d.Q + q] = c_cols[r, 0, q]


def over(x, n):
    return jnp.floor((x.astype(F32) + 0.5) * (1.0 / n)).astype(I32)


def plan_kernel(d, me, gs, gv, inv_ref, cnt_ref, pos_ref, lvl_ref, need, need_send):
    b = gv[:, : d.NB]
    dev = lax.broadcasted_iota(I32, b.shape, 0)
    block = over(dev, d.L)
    lay_of = dev - block * d.L
    col_of = block * d.W + over(lax.broadcasted_iota(I32, b.shape, 1), d.S)
    tri_shape = (d.NB, d.NB)
    tri = jnp.where(
        lax.broadcasted_iota(I32, tri_shape, 0) <= lax.broadcasted_iota(I32, tri_shape, 1), 1.0, 0.0
    )
    most, most_send = jnp.int32(0), jnp.int32(0)

    def per_chip(x):
        return jnp.sum(jnp.sum(x.astype(F32).reshape(d.Y, d.PAIR, d.G * d.L, d.NB), axis=1), axis=2)

    for dst in range(d.Y):

        def one_row(i, acc):
            r = dst * d.PAIR + i // d.RPD
            ci = i % d.RPD
            wanted, wanted_send = None, None
            for h in range(d.L):
                part = None
                for g in range(d.G):
                    for q in range(h * d.QL, (h + 1) * d.QL):
                        hit = col_of == gs[(r * d.G + g) * d.L, d.OFF_C + ci * d.Q + q]
                        part = hit if part is None else part | hit
                away = part & (lay_of != h)
                wanted = part if wanted is None else wanted | part
                wanted_send = away if wanted_send is None else wanted_send | away
            match = None
            base = (r * d.G + ci // d.AR) * d.L
            for s in range(d.SA):
                at = d.NB + (ci % d.AR) * d.SA + s
                want = jnp.full(b.shape, gs[base, at], I32)
                for l in range(1, d.L):
                    want = jnp.where(lay_of == l, gs[base + l, at], want)
                hit = b == want
                match = hit if match is None else match | hit
            return (
                jnp.where(wanted & match, 1, acc[0]),
                jnp.where(wanted_send & match, 1, acc[1]),
            )

        zero = jnp.zeros(b.shape, I32)
        acc, send = lax.fori_loop(0, d.PAIR * d.RPD, one_row, (zero, zero))
        need[dst] = acc
        need_send[dst] = send
        chip = lax.broadcasted_iota(I32, (d.Y, d.G * d.L), 0)
        away = chip != dst
        most = jnp.maximum(most, jnp.max(jnp.where(away, per_chip(acc), 0.0)).astype(I32))
        most_send = jnp.maximum(most_send, jnp.max(jnp.where(away, per_chip(send), 0.0)).astype(I32))
    share = (most + d.PAIR - 1) // d.PAIR
    share_send = (most_send + d.PAIR - 1) // d.PAIR
    level = jnp.int32(0)
    for first, cap in d.caps[:-1]:
        level = level + ((share > cap) | (share_send > first)).astype(I32)
    lvl_ref[0] = level

    y = me[0] // d.PAIR
    mine = me[1] * d.L + me[2]
    lanes = lax.broadcasted_iota(I32, (d.NB, d.PAIR * d.NB), 1).astype(F32)
    ones = jnp.ones((8, d.NB), F32)

    def rows_of(ref, dst, src, c):
        return ref[dst, pl.ds((src * d.PAIR + c) * d.G * d.L + mine, 1), :].astype(F32)

    for delta in range(1, d.Y):
        dst = (y + delta) % d.Y
        src = (y + d.Y - delta) % d.Y
        for kind in range(2):
            before = jnp.float32(0)
            inv = jnp.zeros((1, d.PAIR * d.NB), F32)
            for c in range(d.PAIR):
                bits = rows_of(need_send, dst, y, c)
                if kind == 1:
                    bits = rows_of(need, dst, y, c) - bits
                wide = ones * bits
                upto = lax.dot_general(tri, wide, (((0,), (1,)), ((), ())), preferred_element_type=F32)
                inv = inv + jnp.sum(
                    jnp.where(upto[:, :1] + before <= lanes, 1.0, 0.0), axis=0, keepdims=True
                )
                before = before + jnp.sum(bits)
            inv_ref[delta - 1, kind : kind + 1, :] = inv.astype(I32)
            cnt_ref[delta - 1, kind] = before.astype(I32)
        before = jnp.float32(0)
        position = [None] * d.PAIR
        for kind in range(2):
            for c in range(d.PAIR):
                bits = rows_of(need_send, y, src, c)
                if kind == 1:
                    bits = rows_of(need, y, src, c) - bits
                ahead = jnp.dot(ones * bits, tri, preferred_element_type=F32)[:1] - bits + before
                position[c] = ahead if kind == 0 else jnp.where(bits > 0.5, ahead, position[c])
                before = before + jnp.sum(bits)
        for c in range(d.PAIR):
            pos_ref[delta - 1, c : c + 1, :] = position[c].astype(I32)


def pack_kernel(d, first, cap, me, inv, cnt, own, sib, out, out2, sem):
    core = me[0] % d.PAIR
    total = jnp.int32(0)
    for delta in range(d.Y - 1):
        send = cnt[delta, 0]
        count = (send + cnt[delta, 1] - core + d.PAIR - 1) // d.PAIR

        def one(k, _):
            p = k * d.PAIR + core
            late = jnp.maximum(p - send, 0)
            t = jnp.where(p < send, inv[delta, 0, p], inv[delta, 1, late])
            c = t // d.NB
            t = t % d.NB

            def put(dst):
                @pl.when(c == core)
                def _():
                    pltpu.make_async_copy(own.at[t], dst, sem).start()

                @pl.when(c != core)
                def _():
                    pltpu.make_async_copy(sib.at[t], dst, sem).start()

            @pl.when(k < first)
            def _():
                put(out.at[delta, jnp.minimum(k, first - 1)])

            if cap > first:

                @pl.when(k >= first)
                def _():
                    put(out2.at[delta, jnp.clip(k - first, 0, cap - first - 1)])

            return 0

        lax.fori_loop(0, count, one, 0)
        total = total + count

    def wait(k, _):
        pltpu.make_async_copy(own.at[0], out.at[0, 0], sem).wait()
        return 0

    lax.fori_loop(0, total, wait, 0)


def list_kernel(d, first_cap, me, gs, pos, src_ref, aidx_ref, oidx_ref, starts_ref):
    row, col, lay = me[0], me[1], me[2]
    y = row // d.PAIR
    n = jnp.int32(0)
    for k, (step, low, high, part) in enumerate(d.sections):
        starts_ref[k] = n
        half = (lay + step) % d.L

        def one_pair(i, n):
            sl_d = i // (d.AR * d.QL)
            ar = i // d.QL % d.AR
            qq = i % d.QL
            cc = (col + d.G - (low + sl_d)) % d.G
            ci = cc * d.AR + ar
            j = gs[(row * d.G + col) * d.L + lay, d.OFF_C + ci * d.Q + half * d.QL + qq]
            rp = j // (d.G * d.W)
            w = j % d.W
            a_dev = (row * d.G + cc) * d.L + lay
            a_vals = [gs[a_dev, d.NB + ar * d.SA + s] for s in range(d.SA)]
            a_base = (sl_d * d.AR + ar) * d.SA
            delta = (y + d.Y - rp // d.PAIR) % d.Y
            here = jnp.where(rp == row, 0, d.NB)

            def one_slot(sl, n):
                tile = w * d.S + sl
                b = gs[(rp * d.G + col) * d.L + lay, tile]
                s_hit = jnp.int32(-1)
                for s in range(d.SA):
                    s_hit = jnp.where(b == a_vals[s], s, s_hit)
                there = pos[jnp.maximum(delta - 1, 0), rp % d.PAIR, tile]
                take = s_hit >= 0
                if part is not None:
                    late = (delta != 0) & (there // d.PAIR >= first_cap)
                    take = take & (late == (part == 1))

                @pl.when(take)
                def _():
                    src_ref[n] = jnp.where(delta == 0, here + tile, 2 * d.NB * delta + there)
                    aidx_ref[n] = a_base + s_hit
                    oidx_ref[n] = i

                return n + take.astype(I32)

            return lax.fori_loop(0, d.S, one_slot, n)

        n = lax.fori_loop(0, (high - low) * d.AR * d.QL, one_pair, n)
    starts_ref[len(d.sections)] = n


def product_kernel(d, section, depth, first_cap, n_a, n_x, me, src, aidx, oidx, starts, *refs):
    last = n_x > 0
    n_local = 0 if last else 2
    local, (straight, crossed) = refs[:n_local], refs[n_local : n_local + 2]
    refs = refs[n_local + 2 :]
    a_refs, parts, out = refs[:n_a], refs[n_a : n_a + n_x], refs[n_a + n_x]
    a_all, buf, sem = refs[n_a + n_x + 1 :]
    core = me[0] % d.PAIR
    first = starts[section]
    n = starts[section + 1] - first
    base = first_cap if last else 0
    size = d.AR * d.QL

    def start(k):
        s = src[first + k]
        dst = buf.at[k % depth]
        done = sem.at[k % depth]
        if not last:

            @pl.when(s < d.NB)
            def _():
                pltpu.make_async_copy(local[0].at[jnp.minimum(s, d.NB - 1)], dst, done).start()

            @pl.when((s >= d.NB) & (s < 2 * d.NB))
            def _():
                pltpu.make_async_copy(local[1].at[jnp.clip(s - d.NB, 0, d.NB - 1)], dst, done).start()

        @pl.when(s >= 2 * d.NB)
        def _():
            rest = s - 2 * d.NB
            delta = jnp.minimum(rest // (2 * d.NB), straight.shape[0] - 1)
            p = rest % (2 * d.NB)
            at = jnp.clip(p // d.PAIR - base, 0, straight.shape[1] - 1)

            @pl.when(p % d.PAIR == core)
            def _():
                buf[k % depth] = straight[delta, at]

            @pl.when(p % d.PAIR != core)
            def _():
                buf[k % depth] = crossed[delta, at]

    def start_one(k, _):
        start(k)
        return 0

    lax.fori_loop(0, jnp.minimum(n, depth), start_one, 0)
    rows = d.AR * d.SA
    T = d.T

    @pl.when(n > 0)
    def _():
        for k in range(n_a):
            a = a_refs[k][...]
            hi = a.astype(BF16)
            a_all[k * rows : (k + 1) * rows, :T, :] = hi
            a_all[k * rows : (k + 1) * rows, T:, :] = (a - hi.astype(F32)).astype(BF16)

    def place(slot):
        return (me[1] + d.G - slot) % d.G * size

    if last:
        for k in range(d.G):
            total = parts[0][k * size : (k + 1) * size]
            for m in range((n_x - 1) // 2):
                early, late = parts[1 + 2 * m], parts[2 + 2 * m]
                total = total + (
                    early[k * size : (k + 1) * size]
                    if k < d.EARLY
                    else late[(k - d.EARLY) * size : (k - d.EARLY + 1) * size]
                )
            out[pl.ds(place(k), size)] = total
    else:
        out[...] = jnp.zeros(out.shape, out.dtype)

    def product(k, valid):
        if not last:

            @pl.when(valid & (src[first + k] < 2 * d.NB))
            def _():
                pltpu.make_async_copy(local[0].at[0], buf.at[k % depth], sem.at[k % depth]).wait()

        b = buf[k % depth]
        b = jnp.where(valid, b, 0.0)
        b_hi = b.astype(BF16)
        b_lo = (b - b_hi.astype(F32)).astype(BF16)
        a = a_all[aidx[first + k]]
        both = jnp.dot(a, b_hi, preferred_element_type=F32)
        low = jnp.dot(a[:T], b_lo, preferred_element_type=F32)
        return both[:T] + (both[T:] + low)

    def add(k, value):
        o = oidx[first + k]
        if last:
            o = place(o // size) + o % size
        out[o] = out[o] + value

    def two(i, _):
        k = 2 * i
        valid = k + 1 < n
        k1 = jnp.minimum(k + 1, n - 1)
        p0 = product(k, k < n)
        p1 = product(k1, valid)
        add(k, p0)
        add(k1, p1)
        lax.fori_loop(jnp.minimum(k + depth, n), jnp.minimum(k + depth + 2, n), start_one, 0)
        return 0

    lax.fori_loop(0, (n + 1) // 2, two, 0)


class Dims:
    pass


def on_device(a_tiles, a_cols, b_tiles, b_rows, c_cols):
    d = Dims()
    d.R, d.G, d.L = (lax.axis_size(name) for name in AXES)
    d.W, d.S, d.T = b_tiles.shape[0], b_tiles.shape[2], b_tiles.shape[-1]
    d.AR, d.SA = a_tiles.shape[0], a_tiles.shape[2]
    d.RPD, d.Q = c_cols.shape[0], c_cols.shape[2]
    d.PAIR = 2 if d.R % 2 == 0 else 1
    d.Y, d.NB, d.N, d.QL = d.R // d.PAIR, d.W * d.S, d.R * d.G * d.L, d.Q // d.L
    d.OFF_C = d.NB + d.AR * d.SA
    d.EARLY = 1 + max(1, d.G // 4)
    totals = sorted({-(-d.NB * k // 56) for k in (8, 9, 10, 11, 12, 14, 18, 28)})
    d.caps = tuple((-(-t * 5 // 8), t) for t in totals) + ((d.NB, d.NB),)
    d.sections = tuple(
        (step, low, high, None)
        for step in range(1, d.L)
        for low, high in ((0, d.EARLY), (d.EARLY, d.G))
    ) + ((0, 0, d.G, 0), (0, 0, d.G, 1))
    R, G, L, T, NB, PAIR, Y = d.R, d.G, d.L, d.T, d.NB, d.PAIR, d.Y
    YS = max(Y - 1, 1)
    smem = pl.BlockSpec(memory_space=SMEM)
    vmem = pl.BlockSpec(memory_space=VMEM)
    hbm = pl.BlockSpec(memory_space=HBM)

    def shift(x, k):
        return lax.ppermute(x, "col", [(c, (c + k) % G) for c in range(G)])

    own = b_tiles.reshape(NB, T, T)
    pair_swap = [(r, r ^ (PAIR - 1)) for r in range(R)]
    a_own = a_tiles.reshape(d.AR * d.SA, T, T)
    me = jnp.stack([lax.axis_index(name) for name in AXES]).astype(I32)
    n_idx = d.OFF_C + d.RPD * d.Q

    def limit(*shapes):
        return pltpu.CompilerParams(
            vmem_limit_bytes=(2 << 20) + sum(4 * int(np.prod(shape)) for shape in shapes)
        )

    idx = pl.pallas_call(
        functools.partial(index_kernel, d),
        in_specs=[smem] * 3,
        out_specs=smem,
        out_shape=jax.ShapeDtypeStruct((1, n_idx), I32),
        compiler_params=limit(),
        name="index",
    )(b_rows.transpose(2, 1, 0), a_cols, c_cols)
    group = lax.all_gather(idx, "col", axis=0, tiled=True)
    sib = lax.ppermute(own, "row", pair_swap)
    a_from, group = lax.optimization_barrier((a_own, group))
    a_early = [a_own] + [shift(a_from, k) for k in range(1, d.EARLY)]
    table = lax.all_to_all(
        jnp.broadcast_to(group[None], (R * L, G, n_idx)), ("row", "layer"), 0, 0, tiled=True
    )
    table = table.reshape(R, L, G, n_idx).transpose(0, 2, 1, 3).reshape(d.N, n_idx)

    inv, cnt, pos, level = pl.pallas_call(
        functools.partial(plan_kernel, d),
        in_specs=[smem, smem, vmem],
        out_specs=[vmem, smem, vmem, smem],
        out_shape=[
            jax.ShapeDtypeStruct((YS, 2, PAIR * NB), I32),
            jax.ShapeDtypeStruct((YS, 2), I32),
            jax.ShapeDtypeStruct((YS, PAIR, NB), I32),
            jax.ShapeDtypeStruct((1,), I32),
        ],
        scratch_shapes=[VMEM((Y, d.N, NB), I32)] * 2,
        compiler_params=limit((2 * Y + 8, d.N, 128), (16, 256, 256)),
        name="plan",
    )(me, table, table)

    most = d.RPD * d.Q * d.S

    def run(branch, me, table, inv, cnt, pos, own, sib, *a_early):
        return body(d.caps[branch], me, table, inv, cnt, pos, own, sib, *a_early)

    def body(caps, me, table, inv, cnt, pos, own, sib, *a_early):
        first, cap = caps
        two = cap > first
        second = max(cap - first, 1)
        a_late = [shift(a_early[0], k) for k in range(d.EARLY, G)]
        packs = pl.pallas_call(
            functools.partial(pack_kernel, d, first, cap),
            in_specs=[smem, smem, smem, hbm, hbm],
            out_specs=[vmem, vmem],
            out_shape=[
                jax.ShapeDtypeStruct((YS, first, T, T), F32),
                jax.ShapeDtypeStruct((YS, second, T, T), F32),
            ],
            scratch_shapes=[pltpu.SemaphoreType.DMA],
            compiler_params=limit((YS, first, T, T), (YS, second, T, T)),
            name="pack",
        )(me, inv, cnt, own, sib)

        def across(piece):
            packed = packs[piece]
            recs = [
                lax.ppermute(
                    packed[k - 1 : k],
                    "row",
                    [(r, ((r // PAIR + k) % Y) * PAIR + r % PAIR) for r in range(R)],
                )
                for k in range(1, Y)
            ]
            rec = recs[0] if len(recs) == 1 else jnp.concatenate(recs, 0)
            return [rec, lax.ppermute(rec, "row", pair_swap)]

        received = [across(0), across(1) if two else [packs[1], packs[1]]]
        a_list = list(a_early) + a_late
        src, aidx, oidx, starts = pl.pallas_call(
            functools.partial(list_kernel, d, first),
            in_specs=[smem, smem, smem],
            out_specs=[smem, smem, smem, smem],
            out_shape=[jax.ShapeDtypeStruct((most,), I32)] * 3
            + [jax.ShapeDtypeStruct((len(d.sections) + 1,), I32)],
            compiler_params=limit(),
            cost_estimate=pl.CostEstimate(flops=5 * 10**9, bytes_accessed=10**5, transcendentals=0),
            name="list",
        )(me, table, pos)

        depth = 8

        def products(k, parts=()):
            _, low, high, part = d.sections[k]
            b_local = [] if part == 1 else [own, sib]
            b_far = received[1 if part == 1 else 0]
            a_part = a_list[low:high]
            size = ((high - low) * d.AR * d.QL, T, T)
            n_a = len(a_part) * d.AR * d.SA
            return pl.pallas_call(
                functools.partial(product_kernel, d, k, depth, first, len(a_part), len(parts)),
                in_specs=[smem] * 5
                + [hbm] * len(b_local)
                + [vmem] * (2 + len(a_part) + len(parts)),
                out_specs=vmem,
                out_shape=jax.ShapeDtypeStruct(size, F32),
                scratch_shapes=[
                    VMEM((n_a, 2 * T, T), BF16),
                    VMEM((depth, T, T), F32),
                    pltpu.SemaphoreType.DMA((depth,)),
                ],
                compiler_params=limit(
                    (depth + 2 * n_a, T, T), size, *(x.shape for x in (*b_far, *parts))
                ),
                cost_estimate=pl.CostEstimate(
                    flops=5 * 10**9, bytes_accessed=10**6, transcendentals=0
                ),
                name="products",
            )(me, src, aidx, oidx, starts, *b_local, *b_far, *a_part, *parts)

        moved = []
        for k, (step, _, _, _) in enumerate(d.sections[:-2]):
            part = products(k)
            moved.append(lax.ppermute(part, "layer", [(l, (l + step) % L) for l in range(L)]))
        mine = products(len(d.sections) - 2)
        return products(len(d.sections) - 1, [mine, *moved])

    result = lax.switch(
        level[0],
        [functools.partial(run, k) for k in range(len(d.caps))],
        me, table, inv, cnt, pos, own, sib, *a_early,
    )
    return result.reshape(d.RPD, 1, d.QL, T, T)


def solution(mesh):
    return jax.shard_map(
        on_device,
        mesh=mesh,
        in_specs=(
            P(("row", "col"), "layer", None, None, None),
            P(("row", "col"), "layer", None),
            P(("row", "col"), "layer", None, None, None),
            P(("row", "col"), "layer", None),
            P("row", "col", None),
        ),
        out_specs=P("row", "col", "layer", None, None),
        check_vma=False,
    )
```

```python
import functools

import jax
import jax.numpy as jnp
import numpy as np
from jax import lax
from jax.experimental import pallas as pl
from jax.experimental.pallas import tpu as pltpu
from jax.sharding import PartitionSpec as P


AXES = ("row", "col", "layer")
LADDER = ((10, 18), (11, 20), (12, 22), (13, 24), (14, 26), (16, 28), (20, 36), (36, 64), (112, 112))
SMEM = pltpu.SMEM
VMEM = pltpu.VMEM
HBM = pltpu.HBM
I32 = jnp.int32
F32 = jnp.float32
BF16 = jnp.bfloat16


def index_kernel(d, b_in, a_in, c_in, out, b_rows, a_cols, c_cols, sem):
    pairs = ((b_in, b_rows), (a_in, a_cols), (c_in, c_cols))
    copies = [pltpu.make_async_copy(x, y, sem.at[k]) for k, (x, y) in enumerate(pairs)]
    for copy in copies:
        copy.start()
    for copy in copies:
        copy.wait()
    for w in range(d.W):
        for s in range(d.S):
            out[0, w * d.S + s] = b_rows[s, 0, w]
    for r in range(d.AR):
        for s in range(d.SA):
            out[0, d.NB + r * d.SA + s] = a_cols[r, 0, s]
    for r in range(d.RPD):
        for q in range(d.Q):
            out[0, d.OFF_C + r * d.Q + q] = c_cols[r, 0, q]


def over(x, n):
    return jnp.floor((x.astype(F32) + 0.5) * (1.0 / n)).astype(I32)


def plan_kernel(d, me, gs, gv, inv_ref, cnt_ref, pos_ref, lvl_ref, need, need_send):
    b = gv[:, : d.NB]
    dev = lax.broadcasted_iota(I32, b.shape, 0)
    block = over(dev, d.L)
    lay_of = dev - block * d.L
    col_of = block * d.W + over(lax.broadcasted_iota(I32, b.shape, 1), d.S)
    tri_shape = (d.NB, d.NB)
    tri = jnp.where(
        lax.broadcasted_iota(I32, tri_shape, 0) <= lax.broadcasted_iota(I32, tri_shape, 1), 1.0, 0.0
    )
    most, most_send = jnp.int32(0), jnp.int32(0)

    def per_chip(x):
        return jnp.sum(jnp.sum(x.astype(F32).reshape(d.Y, d.PAIR, d.G * d.L, d.NB), axis=1), axis=2)

    for dst in range(d.Y):

        def one_row(i, acc):
            r = dst * d.PAIR + i // d.RPD
            ci = i % d.RPD
            wanted, wanted_send = None, None
            for h in range(d.L):
                part = None
                for g in range(d.G):
                    for q in range(h * d.QL, (h + 1) * d.QL):
                        hit = col_of == gs[(r * d.G + g) * d.L, d.OFF_C + ci * d.Q + q]
                        part = hit if part is None else part | hit
                away = part & (lay_of != h)
                wanted = part if wanted is None else wanted | part
                wanted_send = away if wanted_send is None else wanted_send | away
            match = None
            base = (r * d.G + ci // d.AR) * d.L
            for s in range(d.SA):
                at = d.NB + (ci % d.AR) * d.SA + s
                want = jnp.full(b.shape, gs[base, at], I32)
                for l in range(1, d.L):
                    want = jnp.where(lay_of == l, gs[base + l, at], want)
                hit = b == want
                match = hit if match is None else match | hit
            return (
                jnp.where(wanted & match, 1, acc[0]),
                jnp.where(wanted_send & match, 1, acc[1]),
            )

        zero = jnp.zeros(b.shape, I32)
        acc, send = lax.fori_loop(0, d.PAIR * d.RPD, one_row, (zero, zero))
        need[dst] = acc
        need_send[dst] = send
        chip = lax.broadcasted_iota(I32, (d.Y, d.G * d.L), 0)
        away = chip != dst
        most = jnp.maximum(most, jnp.max(jnp.where(away, per_chip(acc), 0.0)).astype(I32))
        most_send = jnp.maximum(most_send, jnp.max(jnp.where(away, per_chip(send), 0.0)).astype(I32))
    share = (most + d.PAIR - 1) // d.PAIR
    share_send = (most_send + d.PAIR - 1) // d.PAIR
    level = jnp.int32(0)
    for first, cap in d.caps[:-1]:
        level = level + ((share > cap) | (share_send > first)).astype(I32)
    lvl_ref[0] = level

    y = me[0] // d.PAIR
    mine = me[1] * d.L + me[2]
    lanes = lax.broadcasted_iota(I32, (d.NB, d.PAIR * d.NB), 1).astype(F32)
    ones = jnp.ones((8, d.NB), F32)

    def rows_of(ref, dst, src, c):
        return ref[dst, pl.ds((src * d.PAIR + c) * d.G * d.L + mine, 1), :].astype(F32)

    for delta in range(1, d.Y):
        dst = (y + delta) % d.Y
        src = (y + d.Y - delta) % d.Y
        for kind in range(2):
            before = jnp.float32(0)
            inv = jnp.zeros((1, d.PAIR * d.NB), F32)
            for c in range(d.PAIR):
                bits = rows_of(need_send, dst, y, c)
                if kind == 1:
                    bits = rows_of(need, dst, y, c) - bits
                wide = ones * bits
                upto = lax.dot_general(tri, wide, (((0,), (1,)), ((), ())), preferred_element_type=F32)
                inv = inv + jnp.sum(
                    jnp.where(upto[:, :1] + before <= lanes, 1.0, 0.0), axis=0, keepdims=True
                )
                before = before + jnp.sum(bits)
            inv_ref[delta - 1, kind : kind + 1, :] = inv.astype(I32)
            cnt_ref[delta - 1, kind] = before.astype(I32)
        before = jnp.float32(0)
        position = [None] * d.PAIR
        for kind in range(2):
            for c in range(d.PAIR):
                bits = rows_of(need_send, y, src, c)
                if kind == 1:
                    bits = rows_of(need, y, src, c) - bits
                ahead = jnp.dot(ones * bits, tri, preferred_element_type=F32)[:1] - bits + before
                position[c] = ahead if kind == 0 else jnp.where(bits > 0.5, ahead, position[c])
                before = before + jnp.sum(bits)
        for c in range(d.PAIR):
            pos_ref[delta - 1, c : c + 1, :] = position[c].astype(I32)


def pack_kernel(d, first, cap, me, inv, cnt, own, sib, out, out2, sem):
    core = me[0] % d.PAIR
    total = jnp.int32(0)
    for delta in range(d.Y - 1):
        send = cnt[delta, 0]
        count = (send + cnt[delta, 1] - core + d.PAIR - 1) // d.PAIR

        def one(k, _):
            p = k * d.PAIR + core
            late = jnp.maximum(p - send, 0)
            t = jnp.where(p < send, inv[delta, 0, p], inv[delta, 1, late])
            c = t // d.NB
            t = t % d.NB

            def put(dst):
                @pl.when(c == core)
                def _():
                    pltpu.make_async_copy(own.at[t], dst, sem).start()

                @pl.when(c != core)
                def _():
                    pltpu.make_async_copy(sib.at[t], dst, sem).start()

            @pl.when(k < first)
            def _():
                put(out.at[delta, jnp.minimum(k, first - 1)])

            if cap > first:

                @pl.when(k >= first)
                def _():
                    put(out2.at[delta, jnp.clip(k - first, 0, cap - first - 1)])

            return 0

        lax.fori_loop(0, count, one, 0)
        total = total + count

    def wait(k, _):
        pltpu.make_async_copy(own.at[0], out.at[0, 0], sem).wait()
        return 0

    lax.fori_loop(0, total, wait, 0)


def list_kernel(d, first_cap, me, gs, pos, src_ref, aidx_ref, oidx_ref, starts_ref):
    row, col, lay = me[0], me[1], me[2]
    y = row // d.PAIR
    n = jnp.int32(0)
    for k, (step, low, high, part) in enumerate(d.sections):
        starts_ref[k] = n
        half = (lay + step) % d.L

        def one_pair(i, n):
            sl_d = i // (d.AR * d.QL)
            ar = i // d.QL % d.AR
            qq = i % d.QL
            cc = (col + d.G - (low + sl_d)) % d.G
            ci = cc * d.AR + ar
            j = gs[(row * d.G + col) * d.L + lay, d.OFF_C + ci * d.Q + half * d.QL + qq]
            rp = j // (d.G * d.W)
            w = j % d.W
            a_dev = (row * d.G + cc) * d.L + lay
            a_vals = [gs[a_dev, d.NB + ar * d.SA + s] for s in range(d.SA)]
            a_base = (sl_d * d.AR + ar) * d.SA
            delta = (y + d.Y - rp // d.PAIR) % d.Y
            here = jnp.where(rp == row, 0, d.NB)

            def one_slot(sl, n):
                tile = w * d.S + sl
                b = gs[(rp * d.G + col) * d.L + lay, tile]
                s_hit = jnp.int32(-1)
                for s in range(d.SA):
                    s_hit = jnp.where(b == a_vals[s], s, s_hit)
                there = pos[jnp.maximum(delta - 1, 0), rp % d.PAIR, tile]
                take = s_hit >= 0
                if part is not None:
                    late = (delta != 0) & (there // d.PAIR >= first_cap)
                    take = take & (late == (part == 1))

                @pl.when(take)
                def _():
                    src_ref[n] = jnp.where(delta == 0, here + tile, 2 * d.NB * delta + there)
                    aidx_ref[n] = a_base + s_hit
                    oidx_ref[n] = i

                return n + take.astype(I32)

            return lax.fori_loop(0, d.S, one_slot, n)

        n = lax.fori_loop(0, (high - low) * d.AR * d.QL, one_pair, n)
    starts_ref[len(d.sections)] = n


def product_kernel(d, section, depth, first_cap, n_a, n_x, me, src, aidx, oidx, starts, *refs):
    last = n_x > 0
    n_local = 0 if last else 2
    local, (straight, crossed) = refs[:n_local], refs[n_local : n_local + 2]
    refs = refs[n_local + 2 :]
    a_refs, parts, out = refs[:n_a], refs[n_a : n_a + n_x], refs[n_a + n_x]
    a_all, buf, sem = refs[n_a + n_x + 1 :]
    core = me[0] % d.PAIR
    first = starts[section]
    n = starts[section + 1] - first
    base = first_cap if last else 0
    size = d.AR * d.QL

    def start(k):
        s = src[first + k]
        dst = buf.at[k % depth]
        done = sem.at[k % depth]
        if not last:

            @pl.when(s < d.NB)
            def _():
                pltpu.make_async_copy(local[0].at[jnp.minimum(s, d.NB - 1)], dst, done).start()

            @pl.when((s >= d.NB) & (s < 2 * d.NB))
            def _():
                pltpu.make_async_copy(local[1].at[jnp.clip(s - d.NB, 0, d.NB - 1)], dst, done).start()

        @pl.when(s >= 2 * d.NB)
        def _():
            rest = s - 2 * d.NB
            delta = jnp.minimum(rest // (2 * d.NB), straight.shape[0] - 1)
            p = rest % (2 * d.NB)
            at = jnp.clip(p // d.PAIR - base, 0, straight.shape[1] - 1)

            @pl.when(p % d.PAIR == core)
            def _():
                buf[k % depth] = straight[delta, at]

            @pl.when(p % d.PAIR != core)
            def _():
                buf[k % depth] = crossed[delta, at]

    def start_one(k, _):
        start(k)
        return 0

    lax.fori_loop(0, jnp.minimum(n, depth), start_one, 0)
    rows = d.AR * d.SA
    T = d.T

    @pl.when(n > 0)
    def _():
        for k in range(n_a):
            a = a_refs[k][...]
            hi = a.astype(BF16)
            a_all[k * rows : (k + 1) * rows, :T, :] = hi
            a_all[k * rows : (k + 1) * rows, T:, :] = (a - hi.astype(F32)).astype(BF16)

    def place(slot):
        return (me[1] + d.G - slot) % d.G * size

    if last:
        for k in range(d.G):
            total = parts[0][k * size : (k + 1) * size]
            for m in range((n_x - 1) // 2):
                early, late = parts[1 + 2 * m], parts[2 + 2 * m]
                total = total + (
                    early[k * size : (k + 1) * size]
                    if k < d.EARLY
                    else late[(k - d.EARLY) * size : (k - d.EARLY + 1) * size]
                )
            out[pl.ds(place(k), size)] = total
    else:
        out[...] = jnp.zeros(out.shape, out.dtype)

    def product(k, valid):
        if not last:

            @pl.when(valid & (src[first + k] < 2 * d.NB))
            def _():
                pltpu.make_async_copy(local[0].at[0], buf.at[k % depth], sem.at[k % depth]).wait()

        b = buf[k % depth]
        b = jnp.where(valid, b, 0.0)
        b_hi = b.astype(BF16)
        b_lo = (b - b_hi.astype(F32)).astype(BF16)
        a = a_all[aidx[first + k]]
        both = jnp.dot(a, b_hi, preferred_element_type=F32)
        low = jnp.dot(a[:T], b_lo, preferred_element_type=F32)
        return both[:T] + (both[T:] + low)

    def add(k, value):
        o = oidx[first + k]
        if last:
            o = place(o // size) + o % size
        out[o] = out[o] + value

    def two(i, _):
        k = 2 * i
        valid = k + 1 < n
        k1 = jnp.minimum(k + 1, n - 1)
        p0 = product(k, k < n)
        p1 = product(k1, valid)
        add(k, p0)
        add(k1, p1)
        lax.fori_loop(jnp.minimum(k + depth, n), jnp.minimum(k + depth + 2, n), start_one, 0)
        return 0

    lax.fori_loop(0, (n + 1) // 2, two, 0)


class Dims:
    pass


def on_device(a_tiles, a_cols, b_tiles, b_rows, c_cols):
    d = Dims()
    d.R, d.G, d.L = (lax.axis_size(name) for name in AXES)
    d.W, d.S, d.T = b_tiles.shape[0], b_tiles.shape[2], b_tiles.shape[-1]
    d.AR, d.SA = a_tiles.shape[0], a_tiles.shape[2]
    d.RPD, d.Q = c_cols.shape[0], c_cols.shape[2]
    d.PAIR = 2 if d.R % 2 == 0 else 1
    d.Y, d.NB, d.N, d.QL = d.R // d.PAIR, d.W * d.S, d.R * d.G * d.L, d.Q // d.L
    d.OFF_C = d.NB + d.AR * d.SA
    d.EARLY = 1 + max(1, d.G // 4)
    ladder = {(-(-d.NB * f // 112), -(-d.NB * t // 112)) for f, t in LADDER}
    d.caps = tuple(sorted(ladder))
    d.sections = tuple(
        (step, low, high, None)
        for step in range(1, d.L)
        for low, high in ((0, d.EARLY), (d.EARLY, d.G))
    ) + ((0, 0, d.G, 0), (0, 0, d.G, 1))
    R, G, L, T, NB, PAIR, Y = d.R, d.G, d.L, d.T, d.NB, d.PAIR, d.Y
    YS = max(Y - 1, 1)
    smem = pl.BlockSpec(memory_space=SMEM)
    vmem = pl.BlockSpec(memory_space=VMEM)
    hbm = pl.BlockSpec(memory_space=HBM)

    def shift(x, k):
        return lax.ppermute(x, "col", [(c, (c + k) % G) for c in range(G)])

    own = b_tiles.reshape(NB, T, T)
    pair_swap = [(r, r ^ (PAIR - 1)) for r in range(R)]
    a_own = a_tiles.reshape(d.AR * d.SA, T, T)
    me = jnp.stack([lax.axis_index(name) for name in AXES]).astype(I32)
    n_idx = d.OFF_C + d.RPD * d.Q

    def limit(*shapes):
        return pltpu.CompilerParams(
            vmem_limit_bytes=(2 << 20) + sum(4 * int(np.prod(shape)) for shape in shapes)
        )

    idx = pl.pallas_call(
        functools.partial(index_kernel, d),
        in_specs=[hbm] * 3,
        out_specs=smem,
        out_shape=jax.ShapeDtypeStruct((1, n_idx), I32),
        scratch_shapes=[
            SMEM((d.S, 1, d.W), I32),
            SMEM(a_cols.shape, I32),
            SMEM(c_cols.shape, I32),
            pltpu.SemaphoreType.DMA((3,)),
        ],
        compiler_params=pltpu.CompilerParams(vmem_limit_bytes=60 << 20),
        name="index",
    )(b_rows.transpose(2, 1, 0), a_cols, c_cols)
    group = lax.all_gather(idx, "col", axis=0, tiled=True)
    sib = lax.ppermute(own, "row", pair_swap)
    spread = jnp.broadcast_to(group[None], (R * L, G, n_idx))
    a_from, spread = lax.optimization_barrier((a_own, spread))
    a_early = [a_own] + [shift(a_from, k) for k in range(1, d.EARLY)]
    table = lax.all_to_all(spread, ("row", "layer"), 0, 0, tiled=True)
    table = table.reshape(R, L, G, n_idx).transpose(0, 2, 1, 3).reshape(d.N, n_idx)

    inv, cnt, pos, level = pl.pallas_call(
        functools.partial(plan_kernel, d),
        in_specs=[smem, smem, vmem],
        out_specs=[vmem, smem, vmem, smem],
        out_shape=[
            jax.ShapeDtypeStruct((YS, 2, PAIR * NB), I32),
            jax.ShapeDtypeStruct((YS, 2), I32),
            jax.ShapeDtypeStruct((YS, PAIR, NB), I32),
            jax.ShapeDtypeStruct((1,), I32),
        ],
        scratch_shapes=[VMEM((Y, d.N, NB), I32)] * 2,
        compiler_params=limit((2 * Y + 8, d.N, 128), (16, 256, 256)),
        name="plan",
    )(me, table, table)

    most = d.RPD * d.Q * d.S

    def run(branch, me, table, inv, cnt, pos, own, sib, *a_early):
        return body(d.caps[branch], me, table, inv, cnt, pos, own, sib, *a_early)

    def body(caps, me, table, inv, cnt, pos, own, sib, *a_early):
        first, cap = caps
        two = cap > first
        second = max(cap - first, 1)
        a_late = [shift(a_early[0], k) for k in range(d.EARLY, G)]
        packs = pl.pallas_call(
            functools.partial(pack_kernel, d, first, cap),
            in_specs=[smem, smem, smem, hbm, hbm],
            out_specs=[vmem, vmem],
            out_shape=[
                jax.ShapeDtypeStruct((YS, first, T, T), F32),
                jax.ShapeDtypeStruct((YS, second, T, T), F32),
            ],
            scratch_shapes=[pltpu.SemaphoreType.DMA],
            compiler_params=limit((YS, first, T, T), (YS, second, T, T)),
            name="pack",
        )(me, inv, cnt, own, sib)

        def across(piece):
            packed = packs[piece]
            recs = [
                lax.ppermute(
                    packed[k - 1 : k],
                    "row",
                    [(r, ((r // PAIR + k) % Y) * PAIR + r % PAIR) for r in range(R)],
                )
                for k in range(1, Y)
            ]
            rec = recs[0] if len(recs) == 1 else jnp.concatenate(recs, 0)
            return [rec, lax.ppermute(rec, "row", pair_swap)]

        received = [across(0), across(1) if two else [packs[1], packs[1]]]
        a_list = list(a_early) + a_late
        src, aidx, oidx, starts = pl.pallas_call(
            functools.partial(list_kernel, d, first),
            in_specs=[smem, smem, smem],
            out_specs=[smem, smem, smem, smem],
            out_shape=[jax.ShapeDtypeStruct((most,), I32)] * 3
            + [jax.ShapeDtypeStruct((len(d.sections) + 1,), I32)],
            compiler_params=limit(),
            cost_estimate=pl.CostEstimate(flops=5 * 10**9, bytes_accessed=10**5, transcendentals=0),
            name="list",
        )(me, table, pos)

        depth = 8

        def products(k, parts=()):
            _, low, high, part = d.sections[k]
            b_local = [] if part == 1 else [own, sib]
            b_far = received[1 if part == 1 else 0]
            a_part = a_list[low:high]
            size = ((high - low) * d.AR * d.QL, T, T)
            n_a = len(a_part) * d.AR * d.SA
            return pl.pallas_call(
                functools.partial(product_kernel, d, k, depth, first, len(a_part), len(parts)),
                in_specs=[smem] * 5
                + [hbm] * len(b_local)
                + [vmem] * (2 + len(a_part) + len(parts)),
                out_specs=vmem,
                out_shape=jax.ShapeDtypeStruct(size, F32),
                scratch_shapes=[
                    VMEM((n_a, 2 * T, T), BF16),
                    VMEM((depth, T, T), F32),
                    pltpu.SemaphoreType.DMA((depth,)),
                ],
                compiler_params=limit(
                    (depth + 2 * n_a, T, T), size, *(x.shape for x in (*b_far, *parts))
                ),
                cost_estimate=pl.CostEstimate(
                    flops=5 * 10**9, bytes_accessed=10**6, transcendentals=0
                ),
                name="products",
            )(me, src, aidx, oidx, starts, *b_local, *b_far, *a_part, *parts)

        moved = []
        for k, (step, _, _, _) in enumerate(d.sections[:-2]):
            part = products(k)
            moved.append(lax.ppermute(part, "layer", [(l, (l + step) % L) for l in range(L)]))
        mine = products(len(d.sections) - 2)
        return products(len(d.sections) - 1, [mine, *moved])

    result = lax.switch(
        level[0],
        [functools.partial(run, k) for k in range(len(d.caps))],
        me, table, inv, cnt, pos, own, sib, *a_early,
    )
    return result.reshape(d.RPD, 1, d.QL, T, T)


def solution(mesh):
    return jax.shard_map(
        on_device,
        mesh=mesh,
        in_specs=(
            P(("row", "col"), "layer", None, None, None),
            P(("row", "col"), "layer", None),
            P(("row", "col"), "layer", None, None, None),
            P(("row", "col"), "layer", None),
            P("row", "col", None),
        ),
        out_specs=P("row", "col", "layer", None, None),
        check_vma=False,
    )
```

```python
import functools

import jax
import jax.numpy as jnp
import numpy as np
from jax import lax
from jax.experimental import pallas as pl
from jax.experimental.pallas import tpu as pltpu
from jax.sharding import PartitionSpec as P


AXES = ("row", "col", "layer")
LADDER = ((10, 18), (11, 20), (12, 22), (13, 24), (14, 26), (16, 28), (20, 36), (36, 64), (112, 112))
SMEM = pltpu.SMEM
VMEM = pltpu.VMEM
HBM = pltpu.HBM
I32 = jnp.int32
F32 = jnp.float32
BF16 = jnp.bfloat16


def index_kernel(d, b_in, a_in, c_in, out, b_rows, a_cols, c_cols, sem):
    pairs = ((b_in, b_rows), (a_in, a_cols), (c_in, c_cols))
    copies = [pltpu.make_async_copy(x, y, sem.at[k]) for k, (x, y) in enumerate(pairs)]
    for copy in copies:
        copy.start()
    for copy in copies:
        copy.wait()
    for w in range(d.W):
        for s in range(d.S):
            out[0, w * d.S + s] = b_rows[s, 0, w]
    for r in range(d.AR):
        for s in range(d.SA):
            out[0, d.NB + r * d.SA + s] = a_cols[r, 0, s]
    for r in range(d.RPD):
        for q in range(d.Q):
            out[0, d.OFF_C + r * d.Q + q] = c_cols[r, 0, q]


def over(x, n):
    return jnp.floor((x.astype(F32) + 0.5) * (1.0 / n)).astype(I32)


def shift_of(d, col, slot):
    inner = col > 0
    shift = jnp.where(slot == 1, jnp.where(inner, 1, d.G - 1), slot)
    return jnp.where(slot == d.G - 1, jnp.where(inner, d.G - 1, 1), shift)


def plan_kernel(d, me, gs, gv, inv_ref, cnt_ref, pos_ref, lvl_ref, need, need_send, rows):
    b = gv[:, : d.NB]
    dev = lax.broadcasted_iota(I32, b.shape, 0)
    block = over(dev, d.L)
    lay_of = dev - block * d.L
    col_of = block * d.W + over(lax.broadcasted_iota(I32, b.shape, 1), d.S)
    tri_shape = (d.NB, d.NB)
    tri = jnp.where(
        lax.broadcasted_iota(I32, tri_shape, 0) <= lax.broadcasted_iota(I32, tri_shape, 1), 1.0, 0.0
    )
    most, most_send = jnp.int32(0), jnp.int32(0)

    def per_chip(x):
        return jnp.sum(jnp.sum(x.astype(F32).reshape(d.Y, d.PAIR, d.G * d.L, d.NB), axis=1), axis=2)

    for dst in range(d.Y):

        def one_row(i, acc):
            r = dst * d.PAIR + i // d.RPD
            ci = i % d.RPD
            wanted, wanted_send = None, None
            for h in range(d.L):
                part = None
                for g in range(d.G):
                    for q in range(h * d.QL, (h + 1) * d.QL):
                        hit = col_of == gs[(r * d.G + g) * d.L, d.OFF_C + ci * d.Q + q]
                        part = hit if part is None else part | hit
                away = part & (lay_of != h)
                wanted = part if wanted is None else wanted | part
                wanted_send = away if wanted_send is None else wanted_send | away
            match = None
            base = (r * d.G + ci // d.AR) * d.L
            for s in range(d.SA):
                at = d.NB + (ci % d.AR) * d.SA + s
                want = jnp.full(b.shape, gs[base, at], I32)
                for l in range(1, d.L):
                    want = jnp.where(lay_of == l, gs[base + l, at], want)
                hit = b == want
                match = hit if match is None else match | hit
            return (
                jnp.where(wanted & match, 1, acc[0]),
                jnp.where(wanted_send & match, 1, acc[1]),
            )

        zero = jnp.zeros(b.shape, I32)
        acc, send = lax.fori_loop(0, d.PAIR * d.RPD, one_row, (zero, zero))
        need[dst] = acc
        need_send[dst] = send
        chip = lax.broadcasted_iota(I32, (d.Y, d.G * d.L), 0)
        away = chip != dst
        most = jnp.maximum(most, jnp.max(jnp.where(away, per_chip(acc), 0.0)).astype(I32))
        most_send = jnp.maximum(most_send, jnp.max(jnp.where(away, per_chip(send), 0.0)).astype(I32))
    share = (most + d.PAIR - 1) // d.PAIR
    share_send = (most_send + d.PAIR - 1) // d.PAIR
    level = jnp.int32(0)
    for first, cap in d.caps[:-1]:
        level = level + ((share > cap) | (share_send > first)).astype(I32)
    lvl_ref[0] = level

    y = me[0] // d.PAIR
    mine = me[1] * d.L + me[2]
    lanes = lax.broadcasted_iota(I32, (d.NB, d.PAIR * d.NB), 1).astype(F32)
    width = 2 * d.PAIR

    def rows_of(ref, dst, src, c):
        return ref[dst, pl.ds((src * d.PAIR + c) * d.G * d.L + mine, 1), :].astype(F32)

    rows[...] = jnp.zeros(rows.shape, F32)
    for delta in range(1, d.Y):
        dst = (y + delta) % d.Y
        src = (y + d.Y - delta) % d.Y
        for way, (to, of) in enumerate(((dst, y), (y, src))):
            at = (2 * (delta - 1) + way) * width
            for c in range(d.PAIR):
                send = rows_of(need_send, to, of, c)
                rows[at + c : at + c + 1, :] = send
                rows[at + d.PAIR + c : at + d.PAIR + c + 1, :] = rows_of(need, to, of, c) - send
    bits = rows[...]
    along = jnp.dot(bits, tri, preferred_element_type=F32)
    down = lax.dot_general(tri, bits, (((0,), (1,)), ((), ())), preferred_element_type=F32)
    for delta in range(1, d.Y):
        at = 2 * (delta - 1) * width
        for kind in range(2):
            before = jnp.zeros((1, 1), F32)
            inv = jnp.zeros((1, d.PAIR * d.NB), F32)
            for c in range(d.PAIR):
                r = at + kind * d.PAIR + c
                inv = inv + jnp.sum(
                    jnp.where(down[:, r : r + 1] + before <= lanes, 1.0, 0.0), axis=0, keepdims=True
                )
                before = before + along[r : r + 1, d.NB - 1 : d.NB]
            inv_ref[delta - 1, kind : kind + 1, :] = inv.astype(I32)
            cnt_ref[delta - 1, kind] = jnp.sum(before).astype(I32)
        at = at + width
        before = jnp.zeros((1, 1), F32)
        position = [None] * d.PAIR
        for kind in range(2):
            for c in range(d.PAIR):
                r = at + kind * d.PAIR + c
                ahead = along[r : r + 1] - bits[r : r + 1] + before
                position[c] = ahead if kind == 0 else jnp.where(bits[r : r + 1] > 0.5, ahead, position[c])
                before = before + along[r : r + 1, d.NB - 1 : d.NB]
        for c in range(d.PAIR):
            pos_ref[delta - 1, c : c + 1, :] = position[c].astype(I32)


def pack_kernel(d, first, cap, me, inv, cnt, own, sib, out, out2, sem):
    core = me[0] % d.PAIR
    total = jnp.int32(0)
    for delta in range(d.Y - 1):
        send = cnt[delta, 0]
        count = (send + cnt[delta, 1] - core + d.PAIR - 1) // d.PAIR

        def one(k, _):
            p = k * d.PAIR + core
            late = jnp.maximum(p - send, 0)
            t = jnp.where(p < send, inv[delta, 0, p], inv[delta, 1, late])
            c = t // d.NB
            t = t % d.NB

            def put(dst):
                @pl.when(c == core)
                def _():
                    pltpu.make_async_copy(own.at[t], dst, sem).start()

                @pl.when(c != core)
                def _():
                    pltpu.make_async_copy(sib.at[t], dst, sem).start()

            @pl.when(k < first)
            def _():
                put(out.at[delta, jnp.minimum(k, first - 1)])

            if cap > first:

                @pl.when(k >= first)
                def _():
                    put(out2.at[delta, jnp.clip(k - first, 0, cap - first - 1)])

            return 0

        lax.fori_loop(0, count, one, 0)
        total = total + count

    def wait(k, _):
        pltpu.make_async_copy(own.at[0], out.at[0, 0], sem).wait()
        return 0

    lax.fori_loop(0, total, wait, 0)


def list_kernel(d, first_cap, me, gs, pos, src_ref, aidx_ref, oidx_ref, starts_ref):
    row, col, lay = me[0], me[1], me[2]
    y = row // d.PAIR
    n = jnp.int32(0)
    for k, (step, low, high, part) in enumerate(d.sections):
        starts_ref[k] = n
        half = (lay + step) % d.L

        def one_pair(i, n):
            sl_d = i // (d.AR * d.QL)
            ar = i // d.QL % d.AR
            qq = i % d.QL
            cc = (col + d.G - shift_of(d, col, low + sl_d)) % d.G
            ci = cc * d.AR + ar
            j = gs[(row * d.G + col) * d.L + lay, d.OFF_C + ci * d.Q + half * d.QL + qq]
            rp = j // (d.G * d.W)
            w = j % d.W
            a_dev = (row * d.G + cc) * d.L + lay
            a_vals = [gs[a_dev, d.NB + ar * d.SA + s] for s in range(d.SA)]
            a_base = (sl_d * d.AR + ar) * d.SA
            delta = (y + d.Y - rp // d.PAIR) % d.Y
            here = jnp.where(rp == row, 0, d.NB)

            def one_slot(sl, n):
                tile = w * d.S + sl
                b = gs[(rp * d.G + col) * d.L + lay, tile]
                s_hit = jnp.int32(-1)
                for s in range(d.SA):
                    s_hit = jnp.where(b == a_vals[s], s, s_hit)
                there = pos[jnp.maximum(delta - 1, 0), rp % d.PAIR, tile]
                take = s_hit >= 0
                if part is not None:
                    late = (delta != 0) & (there // d.PAIR >= first_cap)
                    take = take & (late == (part == 1))

                @pl.when(take)
                def _():
                    src_ref[n] = jnp.where(delta == 0, here + tile, 2 * d.NB * delta + there)
                    aidx_ref[n] = a_base + s_hit
                    oidx_ref[n] = i

                return n + take.astype(I32)

            return lax.fori_loop(0, d.S, one_slot, n)

        n = lax.fori_loop(0, (high - low) * d.AR * d.QL, one_pair, n)
    starts_ref[len(d.sections)] = n


def product_kernel(d, section, depth, first_cap, a_fill, n_x, me, src, aidx, oidx, starts, *refs):
    last = n_x > 0
    n_local = 0 if last else 2
    local, (straight, crossed) = refs[:n_local], refs[n_local : n_local + 2]
    refs = refs[n_local + 2 :]
    n_a = len(a_fill)
    a_refs, parts, out = refs[:n_a], refs[n_a : n_a + n_x], refs[n_a + n_x]
    a_all, buf, sem = refs[n_a + n_x + 1 :]
    core = me[0] % d.PAIR
    first = starts[section]
    n = starts[section + 1] - first
    base = first_cap if last else 0
    size = d.AR * d.QL

    def start(k):
        s = src[first + k]
        dst = buf.at[k % depth]
        done = sem.at[k % depth]
        if not last:

            @pl.when(s < d.NB)
            def _():
                pltpu.make_async_copy(local[0].at[jnp.minimum(s, d.NB - 1)], dst, done).start()

            @pl.when((s >= d.NB) & (s < 2 * d.NB))
            def _():
                pltpu.make_async_copy(local[1].at[jnp.clip(s - d.NB, 0, d.NB - 1)], dst, done).start()

        @pl.when(s >= 2 * d.NB)
        def _():
            rest = s - 2 * d.NB
            delta = jnp.minimum(rest // (2 * d.NB), straight.shape[0] - 1)
            p = rest % (2 * d.NB)
            at = jnp.clip(p // d.PAIR - base, 0, straight.shape[1] - 1)

            @pl.when(p % d.PAIR == core)
            def _():
                buf[k % depth] = straight[delta, at]

            @pl.when(p % d.PAIR != core)
            def _():
                buf[k % depth] = crossed[delta, at]

    def start_one(k, _):
        start(k)
        return 0

    lax.fori_loop(0, jnp.minimum(n, depth), start_one, 0)
    rows = d.AR * d.SA
    T = d.T

    col = me[1]
    for ref, uses in zip(a_refs, a_fill, strict=True):
        active, slot = n < 0, jnp.int32(0)
        for use, low, high in uses:
            here = (col >= low) & (col < high)
            active = active | here
            slot = jnp.where(here, use, slot)

        def split(r, _):
            a = ref[r]
            hi = a.astype(BF16)
            a_all[slot * rows + r, :T, :] = hi
            a_all[slot * rows + r, T:, :] = (a - hi.astype(F32)).astype(BF16)
            return 0

        lax.fori_loop(0, jnp.where(active & (n > 0), rows, 0), split, 0)

    def place(slot):
        return (me[1] + d.G - shift_of(d, me[1], slot)) % d.G * size

    if last:
        for k in range(d.G):
            total = parts[0][k * size : (k + 1) * size]
            for m in range((n_x - 1) // 2):
                early, late = parts[1 + 2 * m], parts[2 + 2 * m]
                total = total + (
                    early[k * size : (k + 1) * size]
                    if k < d.EARLY
                    else late[(k - d.EARLY) * size : (k - d.EARLY + 1) * size]
                )
            out[pl.ds(place(k), size)] = total
    else:
        out[...] = jnp.zeros(out.shape, out.dtype)

    def product(k, valid):
        if not last:

            @pl.when(valid & (src[first + k] < 2 * d.NB))
            def _():
                pltpu.make_async_copy(local[0].at[0], buf.at[k % depth], sem.at[k % depth]).wait()

        b = buf[k % depth]
        b = jnp.where(valid, b, 0.0)
        b_hi = b.astype(BF16)
        b_lo = (b - b_hi.astype(F32)).astype(BF16)
        a = a_all[aidx[first + k]]
        both = jnp.dot(a, b_hi, preferred_element_type=F32)
        low = jnp.dot(a[:T], b_lo, preferred_element_type=F32)
        return both[:T] + (both[T:] + low)

    def add(k, value):
        o = oidx[first + k]
        if last:
            o = place(o // size) + o % size
        out[o] = out[o] + value

    def two(i, _):
        k = 2 * i
        valid = k + 1 < n
        k1 = jnp.minimum(k + 1, n - 1)
        p0 = product(k, k < n)
        p1 = product(k1, valid)
        add(k, p0)
        add(k1, p1)
        lax.fori_loop(jnp.minimum(k + depth, n), jnp.minimum(k + depth + 2, n), start_one, 0)
        return 0

    lax.fori_loop(0, (n + 1) // 2, two, 0)


class Dims:
    pass


def on_device(a_tiles, a_cols, b_tiles, b_rows, c_cols):
    d = Dims()
    d.R, d.G, d.L = (lax.axis_size(name) for name in AXES)
    d.W, d.S, d.T = b_tiles.shape[0], b_tiles.shape[2], b_tiles.shape[-1]
    d.AR, d.SA = a_tiles.shape[0], a_tiles.shape[2]
    d.RPD, d.Q = c_cols.shape[0], c_cols.shape[2]
    d.PAIR = 2 if d.R % 2 == 0 else 1
    d.Y, d.NB, d.N, d.QL = d.R // d.PAIR, d.W * d.S, d.R * d.G * d.L, d.Q // d.L
    d.OFF_C = d.NB + d.AR * d.SA
    d.EARLY = 2
    ladder = {(-(-d.NB * f // 112), -(-d.NB * t // 112)) for f, t in LADDER}
    d.caps = tuple(sorted(ladder))
    d.sections = tuple(
        (step, low, high, None)
        for step in range(1, d.L)
        for low, high in ((0, d.EARLY), (d.EARLY, d.G))
    ) + ((0, 0, d.G, 0), (0, 0, d.G, 1))
    R, G, L, T, NB, PAIR, Y = d.R, d.G, d.L, d.T, d.NB, d.PAIR, d.Y
    YS = max(Y - 1, 1)
    smem = pl.BlockSpec(memory_space=SMEM)
    vmem = pl.BlockSpec(memory_space=VMEM)
    hbm = pl.BlockSpec(memory_space=HBM)

    def move(x, pairs):
        return lax.ppermute(x, "col", [(c, t) for c, t in pairs if 0 <= t < G])

    own = b_tiles.reshape(NB, T, T)
    pair_swap = [(r, r ^ (PAIR - 1)) for r in range(R)]
    a_own = a_tiles.reshape(d.AR * d.SA, T, T)
    me = jnp.stack([lax.axis_index(name) for name in AXES]).astype(I32)
    n_idx = d.OFF_C + d.RPD * d.Q

    def limit(*shapes):
        return pltpu.CompilerParams(
            vmem_limit_bytes=(2 << 20) + sum(4 * int(np.prod(shape)) for shape in shapes)
        )

    idx = pl.pallas_call(
        functools.partial(index_kernel, d),
        in_specs=[hbm] * 3,
        out_specs=smem,
        out_shape=jax.ShapeDtypeStruct((1, n_idx), I32),
        scratch_shapes=[
            SMEM((d.S, 1, d.W), I32),
            SMEM(a_cols.shape, I32),
            SMEM(c_cols.shape, I32),
            pltpu.SemaphoreType.DMA((3,)),
        ],
        compiler_params=pltpu.CompilerParams(vmem_limit_bytes=60 << 20),
        name="index",
    )(b_rows.transpose(2, 1, 0), a_cols, c_cols)
    group = lax.all_gather(idx, "col", axis=0, tiled=True)
    sib = lax.ppermute(own, "row", pair_swap)
    spread = jnp.broadcast_to(group[None], (R * L, G, n_idx))
    a_from, spread = lax.optimization_barrier((a_own, spread))
    up = move(a_from, [(c, c + 1) for c in range(G)])
    down = move(a_from, [(c, c - 1) for c in range(G)])
    a_early = [a_own, up, down]
    table = lax.all_to_all(spread, ("row", "layer"), 0, 0, tiled=True)
    table = table.reshape(R, L, G, n_idx).transpose(0, 2, 1, 3).reshape(d.N, n_idx)

    inv, cnt, pos, level = pl.pallas_call(
        functools.partial(plan_kernel, d),
        in_specs=[smem, smem, vmem],
        out_specs=[vmem, smem, vmem, smem],
        out_shape=[
            jax.ShapeDtypeStruct((YS, 2, PAIR * NB), I32),
            jax.ShapeDtypeStruct((YS, 2), I32),
            jax.ShapeDtypeStruct((YS, PAIR, NB), I32),
            jax.ShapeDtypeStruct((1,), I32),
        ],
        scratch_shapes=[VMEM((Y, d.N, NB), I32)] * 2 + [VMEM((YS * 4 * PAIR, NB), F32)],
        compiler_params=limit((2 * Y + 8, d.N, 128), (16, 256, 256)),
        name="plan",
    )(me, table, table)

    most = d.RPD * d.Q * d.S

    def run(branch, me, table, inv, cnt, pos, own, sib, *a_early):
        return body(d.caps[branch], me, table, inv, cnt, pos, own, sib, *a_early)

    def body(caps, me, table, inv, cnt, pos, own, sib, *a_early):
        first, cap = caps
        two = cap > first
        second = max(cap - first, 1)
        a_own, up, down = a_early
        ends = move(a_own, [(0, G - 1), (G - 1, 0)])
        a_slots = [
            (a_own, [(0, 0, G)]),
            (up, [(1, 1, G)]),
            (down, [(1, 0, 1), (G - 1, 1, G - 1)]),
            (ends, [(G - 1, 0, 1), (G - 1, G - 1, G)]),
        ]
        for k in range(2, G - 1):
            back = G - k
            if k == 2:
                a_slots.append((move(up, [(c, c + 1) for c in range(1, G)]), [(k, k, G)]))
            if back == 2:
                a_slots.append((move(down, [(c, c - 1) for c in range(G - 1)]), [(k, 0, k)]))
            direct = [(c, c + k) for c in range(G)] if k != 2 else []
            direct += [(c, c - back) for c in range(G)] if back != 2 else []
            if direct:
                low, high = (k if back == 2 else 0), (k if k == 2 else G)
                a_slots.append((move(a_own, direct), [(k, low, high)]))
        packs = pl.pallas_call(
            functools.partial(pack_kernel, d, first, cap),
            in_specs=[smem, smem, smem, hbm, hbm],
            out_specs=[vmem, vmem],
            out_shape=[
                jax.ShapeDtypeStruct((YS, first, T, T), F32),
                jax.ShapeDtypeStruct((YS, second, T, T), F32),
            ],
            scratch_shapes=[pltpu.SemaphoreType.DMA],
            compiler_params=limit((YS, first, T, T), (YS, second, T, T)),
            name="pack",
        )(me, inv, cnt, own, sib)

        def across(piece):
            packed = packs[piece]
            recs = [
                lax.ppermute(
                    packed[k - 1 : k],
                    "row",
                    [(r, ((r // PAIR + k) % Y) * PAIR + r % PAIR) for r in range(R)],
                )
                for k in range(1, Y)
            ]
            rec = recs[0] if len(recs) == 1 else jnp.concatenate(recs, 0)
            return [rec, lax.ppermute(rec, "row", pair_swap)]

        received = [across(0), across(1) if two else [packs[1], packs[1]]]
        src, aidx, oidx, starts = pl.pallas_call(
            functools.partial(list_kernel, d, first),
            in_specs=[smem, smem, smem],
            out_specs=[smem, smem, smem, smem],
            out_shape=[jax.ShapeDtypeStruct((most,), I32)] * 3
            + [jax.ShapeDtypeStruct((len(d.sections) + 1,), I32)],
            compiler_params=limit(),
            cost_estimate=pl.CostEstimate(flops=5 * 10**9, bytes_accessed=10**5, transcendentals=0),
            name="list",
        )(me, table, pos)

        depth = 8

        def products(k, parts=()):
            _, low, high, part = d.sections[k]
            b_local = [] if part == 1 else [own, sib]
            b_far = received[1 if part == 1 else 0]
            chosen = [
                (x, tuple((use - low, c0, c1) for use, c0, c1 in uses if low <= use < high))
                for x, uses in a_slots
            ]
            a_part = [x for x, uses in chosen if uses]
            a_fill = tuple(uses for _, uses in chosen if uses)
            size = ((high - low) * d.AR * d.QL, T, T)
            n_a = (high - low) * d.AR * d.SA
            return pl.pallas_call(
                functools.partial(product_kernel, d, k, depth, first, a_fill, len(parts)),
                in_specs=[smem] * 5
                + [hbm] * len(b_local)
                + [vmem] * (2 + len(a_part) + len(parts)),
                out_specs=vmem,
                out_shape=jax.ShapeDtypeStruct(size, F32),
                scratch_shapes=[
                    VMEM((n_a, 2 * T, T), BF16),
                    VMEM((depth, T, T), F32),
                    pltpu.SemaphoreType.DMA((depth,)),
                ],
                compiler_params=limit(
                    (depth + n_a + len(a_part) * d.AR * d.SA, T, T), size, *(x.shape for x in (*b_far, *parts))
                ),
                cost_estimate=pl.CostEstimate(
                    flops=5 * 10**9, bytes_accessed=10**6, transcendentals=0
                ),
                name="products",
            )(me, src, aidx, oidx, starts, *b_local, *b_far, *a_part, *parts)

        moved = []
        for k, (step, _, _, _) in enumerate(d.sections[:-2]):
            part = products(k)
            moved.append(lax.ppermute(part, "layer", [(l, (l + step) % L) for l in range(L)]))
        mine = products(len(d.sections) - 2)
        return products(len(d.sections) - 1, [mine, *moved])

    result = lax.switch(
        level[0],
        [functools.partial(run, k) for k in range(len(d.caps))],
        me, table, inv, cnt, pos, own, sib, *a_early,
    )
    return result.reshape(d.RPD, 1, d.QL, T, T)


def solution(mesh):
    return jax.shard_map(
        on_device,
        mesh=mesh,
        in_specs=(
            P(("row", "col"), "layer", None, None, None),
            P(("row", "col"), "layer", None),
            P(("row", "col"), "layer", None, None, None),
            P(("row", "col"), "layer", None),
            P("row", "col", None),
        ),
        out_specs=P("row", "col", "layer", None, None),
        check_vma=False,
    )
```

```python
import functools

import jax
import jax.numpy as jnp
import numpy as np
from jax import lax
from jax.experimental import pallas as pl
from jax.experimental.pallas import tpu as pltpu
from jax.sharding import PartitionSpec as P


AXES = ("row", "col", "layer")
LADDER = ((10, 18), (11, 20), (12, 22), (13, 24), (14, 26), (16, 28), (20, 36), (36, 64), (112, 112))
SMEM = pltpu.SMEM
VMEM = pltpu.VMEM
HBM = pltpu.HBM
I32 = jnp.int32
F32 = jnp.float32
BF16 = jnp.bfloat16


def index_kernel(d, b_in, a_in, c_in, out, b_rows, a_cols, c_cols, sem):
    pairs = ((b_in, b_rows), (a_in, a_cols), (c_in, c_cols))
    copies = [pltpu.make_async_copy(x, y, sem.at[k]) for k, (x, y) in enumerate(pairs)]
    for copy in copies:
        copy.start()
    for copy in copies:
        copy.wait()
    for w in range(d.W):
        for s in range(d.S):
            out[0, w * d.S + s] = b_rows[s, 0, w]
    for r in range(d.AR):
        for s in range(d.SA):
            out[0, d.NB + r * d.SA + s] = a_cols[r, 0, s]
    for r in range(d.RPD):
        for q in range(d.Q):
            out[0, d.OFF_C + r * d.Q + q] = c_cols[r, 0, q]


def over(x, n):
    return jnp.floor((x.astype(F32) + 0.5) * (1.0 / n)).astype(I32)


def plan_kernel(d, me, gs, gv, inv_ref, cnt_ref, pos_ref, lvl_ref, need, need_send):
    b = gv[:, : d.NB]
    dev = lax.broadcasted_iota(I32, b.shape, 0)
    block = over(dev, d.L)
    lay_of = dev - block * d.L
    col_of = block * d.W + over(lax.broadcasted_iota(I32, b.shape, 1), d.S)
    tri_shape = (d.NB, d.NB)
    tri = jnp.where(
        lax.broadcasted_iota(I32, tri_shape, 0) <= lax.broadcasted_iota(I32, tri_shape, 1), 1.0, 0.0
    )
    most, most_send = jnp.int32(0), jnp.int32(0)

    def per_chip(x):
        return jnp.sum(jnp.sum(x.astype(F32).reshape(d.Y, d.PAIR, d.G * d.L, d.NB), axis=1), axis=2)

    for dst in range(d.Y):

        def one_row(i, acc):
            r = dst * d.PAIR + i // d.RPD
            ci = i % d.RPD
            wanted, wanted_send = None, None
            for h in range(d.L):
                part = None
                for g in range(d.G):
                    for q in range(h * d.QL, (h + 1) * d.QL):
                        hit = col_of == gs[(r * d.G + g) * d.L, d.OFF_C + ci * d.Q + q]
                        part = hit if part is None else part | hit
                away = part & (lay_of != h)
                wanted = part if wanted is None else wanted | part
                wanted_send = away if wanted_send is None else wanted_send | away
            match = None
            base = (r * d.G + ci // d.AR) * d.L
            for s in range(d.SA):
                at = d.NB + (ci % d.AR) * d.SA + s
                want = jnp.full(b.shape, gs[base, at], I32)
                for l in range(1, d.L):
                    want = jnp.where(lay_of == l, gs[base + l, at], want)
                hit = b == want
                match = hit if match is None else match | hit
            return (
                jnp.where(wanted & match, 1, acc[0]),
                jnp.where(wanted_send & match, 1, acc[1]),
            )

        zero = jnp.zeros(b.shape, I32)
        acc, send = lax.fori_loop(0, d.PAIR * d.RPD, one_row, (zero, zero))
        need[dst] = acc
        need_send[dst] = send
        chip = lax.broadcasted_iota(I32, (d.Y, d.G * d.L), 0)
        away = chip != dst
        most = jnp.maximum(most, jnp.max(jnp.where(away, per_chip(acc), 0.0)).astype(I32))
        most_send = jnp.maximum(most_send, jnp.max(jnp.where(away, per_chip(send), 0.0)).astype(I32))
    share = (most + d.PAIR - 1) // d.PAIR
    share_send = (most_send + d.PAIR - 1) // d.PAIR
    level = jnp.int32(0)
    for first, cap in d.caps[:-1]:
        level = level + ((share > cap) | (share_send > first)).astype(I32)
    lvl_ref[0] = level

    y = me[0] // d.PAIR
    mine = me[1] * d.L + me[2]
    lanes = lax.broadcasted_iota(I32, (d.NB, d.PAIR * d.NB), 1).astype(F32)
    ones = jnp.ones((8, d.NB), F32)

    def rows_of(ref, dst, src, c):
        return ref[dst, pl.ds((src * d.PAIR + c) * d.G * d.L + mine, 1), :].astype(F32)

    for delta in range(1, d.Y):
        dst = (y + delta) % d.Y
        src = (y + d.Y - delta) % d.Y
        for kind in range(2):
            before = jnp.float32(0)
            inv = jnp.zeros((1, d.PAIR * d.NB), F32)
            for c in range(d.PAIR):
                bits = rows_of(need_send, dst, y, c)
                if kind == 1:
                    bits = rows_of(need, dst, y, c) - bits
                wide = ones * bits
                upto = lax.dot_general(tri, wide, (((0,), (1,)), ((), ())), preferred_element_type=F32)
                inv = inv + jnp.sum(
                    jnp.where(upto[:, :1] + before <= lanes, 1.0, 0.0), axis=0, keepdims=True
                )
                before = before + jnp.sum(bits)
            inv_ref[delta - 1, kind : kind + 1, :] = inv.astype(I32)
            cnt_ref[delta - 1, kind] = before.astype(I32)
        before = jnp.float32(0)
        position = [None] * d.PAIR
        for kind in range(2):
            for c in range(d.PAIR):
                bits = rows_of(need_send, y, src, c)
                if kind == 1:
                    bits = rows_of(need, y, src, c) - bits
                ahead = jnp.dot(ones * bits, tri, preferred_element_type=F32)[:1] - bits + before
                position[c] = ahead if kind == 0 else jnp.where(bits > 0.5, ahead, position[c])
                before = before + jnp.sum(bits)
        for c in range(d.PAIR):
            pos_ref[delta - 1, c : c + 1, :] = position[c].astype(I32)


def pack_kernel(d, first, cap, me, inv, cnt, own, sib, out, out2, sem):
    core = me[0] % d.PAIR
    total = jnp.int32(0)
    for delta in range(d.Y - 1):
        send = cnt[delta, 0]
        count = (send + cnt[delta, 1] - core + d.PAIR - 1) // d.PAIR

        def one(k, _):
            p = k * d.PAIR + core
            late = jnp.maximum(p - send, 0)
            t = jnp.where(p < send, inv[delta, 0, p], inv[delta, 1, late])
            c = t // d.NB
            t = t % d.NB

            def put(dst):
                @pl.when(c == core)
                def _():
                    pltpu.make_async_copy(own.at[t], dst, sem).start()

                @pl.when(c != core)
                def _():
                    pltpu.make_async_copy(sib.at[t], dst, sem).start()

            @pl.when(k < first)
            def _():
                put(out.at[delta, jnp.minimum(k, first - 1)])

            if cap > first:

                @pl.when(k >= first)
                def _():
                    put(out2.at[delta, jnp.clip(k - first, 0, cap - first - 1)])

            return 0

        lax.fori_loop(0, count, one, 0)
        total = total + count

    def wait(k, _):
        pltpu.make_async_copy(own.at[0], out.at[0, 0], sem).wait()
        return 0

    lax.fori_loop(0, total, wait, 0)


def list_kernel(d, first_cap, me, gs, pos, src_ref, aidx_ref, oidx_ref, starts_ref):
    row, col, lay = me[0], me[1], me[2]
    y = row // d.PAIR
    n = jnp.int32(0)
    for k, (step, low, high, part) in enumerate(d.sections):
        starts_ref[k] = n
        half = (lay + step) % d.L

        def one_pair(i, n):
            sl_d = i // (d.AR * d.QL)
            ar = i // d.QL % d.AR
            qq = i % d.QL
            cc = (col + d.G - (low + sl_d)) % d.G
            ci = cc * d.AR + ar
            j = gs[(row * d.G + col) * d.L + lay, d.OFF_C + ci * d.Q + half * d.QL + qq]
            rp = j // (d.G * d.W)
            w = j % d.W
            a_dev = (row * d.G + cc) * d.L + lay
            a_vals = [gs[a_dev, d.NB + ar * d.SA + s] for s in range(d.SA)]
            a_base = (sl_d * d.AR + ar) * d.SA
            delta = (y + d.Y - rp // d.PAIR) % d.Y
            here = jnp.where(rp == row, 0, d.NB)

            def one_slot(sl, n):
                tile = w * d.S + sl
                b = gs[(rp * d.G + col) * d.L + lay, tile]
                s_hit = jnp.int32(-1)
                for s in range(d.SA):
                    s_hit = jnp.where(b == a_vals[s], s, s_hit)
                there = pos[jnp.maximum(delta - 1, 0), rp % d.PAIR, tile]
                take = s_hit >= 0
                if part is not None:
                    late = (delta != 0) & (there // d.PAIR >= first_cap)
                    take = take & (late == (part == 1))

                @pl.when(take)
                def _():
                    src_ref[n] = jnp.where(delta == 0, here + tile, 2 * d.NB * delta + there)
                    aidx_ref[n] = a_base + s_hit
                    oidx_ref[n] = i

                return n + take.astype(I32)

            return lax.fori_loop(0, d.S, one_slot, n)

        n = lax.fori_loop(0, (high - low) * d.AR * d.QL, one_pair, n)
    starts_ref[len(d.sections)] = n


def product_kernel(d, section, depth, first_cap, n_a, n_x, me, src, aidx, oidx, starts, *refs):
    last = n_x > 0
    n_local = 0 if last else 2
    local, (straight, crossed) = refs[:n_local], refs[n_local : n_local + 2]
    refs = refs[n_local + 2 :]
    a_refs, parts, out = refs[:n_a], refs[n_a : n_a + n_x], refs[n_a + n_x]
    a_all, buf, sem = refs[n_a + n_x + 1 :]
    core = me[0] % d.PAIR
    first = starts[section]
    n = starts[section + 1] - first
    base = first_cap if last else 0
    size = d.AR * d.QL

    def start(k):
        s = src[first + k]
        dst = buf.at[k % depth]
        done = sem.at[k % depth]
        if not last:

            @pl.when(s < d.NB)
            def _():
                pltpu.make_async_copy(local[0].at[jnp.minimum(s, d.NB - 1)], dst, done).start()

            @pl.when((s >= d.NB) & (s < 2 * d.NB))
            def _():
                pltpu.make_async_copy(local[1].at[jnp.clip(s - d.NB, 0, d.NB - 1)], dst, done).start()

        @pl.when(s >= 2 * d.NB)
        def _():
            rest = s - 2 * d.NB
            delta = jnp.minimum(rest // (2 * d.NB), straight.shape[0] - 1)
            p = rest % (2 * d.NB)
            at = jnp.clip(p // d.PAIR - base, 0, straight.shape[1] - 1)

            @pl.when(p % d.PAIR == core)
            def _():
                buf[k % depth] = straight[delta, at]

            @pl.when(p % d.PAIR != core)
            def _():
                buf[k % depth] = crossed[delta, at]

    def start_one(k, _):
        start(k)
        return 0

    lax.fori_loop(0, jnp.minimum(n, depth), start_one, 0)
    rows = d.AR * d.SA
    T = d.T

    @pl.when(n > 0)
    def _():
        for k in range(n_a):
            a = a_refs[k][...]
            hi = a.astype(BF16)
            a_all[k * rows : (k + 1) * rows, :T, :] = hi
            a_all[k * rows : (k + 1) * rows, T:, :] = (a - hi.astype(F32)).astype(BF16)

    def place(slot):
        return (me[1] + d.G - slot) % d.G * size

    if last:
        for k in range(d.G):
            total = parts[0][k * size : (k + 1) * size]
            for m in range((n_x - 1) // 2):
                early, late = parts[1 + 2 * m], parts[2 + 2 * m]
                total = total + (
                    early[k * size : (k + 1) * size]
                    if k < d.EARLY
                    else late[(k - d.EARLY) * size : (k - d.EARLY + 1) * size]
                )
            out[pl.ds(place(k), size)] = total
    else:
        out[...] = jnp.zeros(out.shape, out.dtype)

    def product(k, valid):
        if not last:

            @pl.when(valid & (src[first + k] < 2 * d.NB))
            def _():
                pltpu.make_async_copy(local[0].at[0], buf.at[k % depth], sem.at[k % depth]).wait()

        b = buf[k % depth]
        b = jnp.where(valid, b, 0.0)
        b_hi = b.astype(BF16)
        b_lo = (b - b_hi.astype(F32)).astype(BF16)
        a = a_all[aidx[first + k]]
        both = jnp.dot(a, b_hi, preferred_element_type=F32)
        low = jnp.dot(a[:T], b_lo, preferred_element_type=F32)
        return both[:T] + (both[T:] + low)

    def add(k, value):
        o = oidx[first + k]
        if last:
            o = place(o // size) + o % size
        out[o] = out[o] + value

    def two(i, _):
        k = 2 * i
        valid = k + 1 < n
        k1 = jnp.minimum(k + 1, n - 1)
        p0 = product(k, k < n)
        p1 = product(k1, valid)
        add(k, p0)
        add(k1, p1)
        lax.fori_loop(jnp.minimum(k + depth, n), jnp.minimum(k + depth + 2, n), start_one, 0)
        return 0

    lax.fori_loop(0, (n + 1) // 2, two, 0)


class Dims:
    pass


def on_device(a_tiles, a_cols, b_tiles, b_rows, c_cols):
    d = Dims()
    d.R, d.G, d.L = (lax.axis_size(name) for name in AXES)
    d.W, d.S, d.T = b_tiles.shape[0], b_tiles.shape[2], b_tiles.shape[-1]
    d.AR, d.SA = a_tiles.shape[0], a_tiles.shape[2]
    d.RPD, d.Q = c_cols.shape[0], c_cols.shape[2]
    d.PAIR = 2 if d.R % 2 == 0 else 1
    d.Y, d.NB, d.N, d.QL = d.R // d.PAIR, d.W * d.S, d.R * d.G * d.L, d.Q // d.L
    d.OFF_C = d.NB + d.AR * d.SA
    d.EARLY = 1 + max(1, d.G // 4)
    ladder = {(-(-d.NB * f // 112), -(-d.NB * t // 112)) for f, t in LADDER}
    d.caps = tuple(sorted(ladder))
    d.sections = tuple(
        (step, low, high, None)
        for step in range(1, d.L)
        for low, high in ((0, d.EARLY), (d.EARLY, d.G))
    ) + ((0, 0, d.G, 0), (0, 0, d.G, 1))
    R, G, L, T, NB, PAIR, Y = d.R, d.G, d.L, d.T, d.NB, d.PAIR, d.Y
    YS = max(Y - 1, 1)
    smem = pl.BlockSpec(memory_space=SMEM)
    vmem = pl.BlockSpec(memory_space=VMEM)
    hbm = pl.BlockSpec(memory_space=HBM)

    def shift(x, k):
        return lax.ppermute(x, "col", [(c, (c + k) % G) for c in range(G)])

    own = b_tiles.reshape(NB, T, T)
    pair_swap = [(r, r ^ (PAIR - 1)) for r in range(R)]
    a_own = a_tiles.reshape(d.AR * d.SA, T, T)
    me = jnp.stack([lax.axis_index(name) for name in AXES]).astype(I32)
    n_idx = d.OFF_C + d.RPD * d.Q

    def limit(*shapes):
        return pltpu.CompilerParams(
            vmem_limit_bytes=(2 << 20) + sum(4 * int(np.prod(shape)) for shape in shapes)
        )

    idx = pl.pallas_call(
        functools.partial(index_kernel, d),
        in_specs=[hbm] * 3,
        out_specs=smem,
        out_shape=jax.ShapeDtypeStruct((1, n_idx), I32),
        scratch_shapes=[
            SMEM((d.S, 1, d.W), I32),
            SMEM(a_cols.shape, I32),
            SMEM(c_cols.shape, I32),
            pltpu.SemaphoreType.DMA((3,)),
        ],
        compiler_params=pltpu.CompilerParams(vmem_limit_bytes=60 << 20),
        name="index",
    )(b_rows.transpose(2, 1, 0), a_cols, c_cols)
    group = lax.all_gather(idx, "col", axis=0, tiled=True)
    sib = lax.ppermute(own, "row", pair_swap)
    spread = jnp.broadcast_to(group[None], (R * L, G, n_idx))
    a_from, spread = lax.optimization_barrier((a_own, spread))
    a_early = [a_own] + [shift(a_from, k) for k in range(1, d.EARLY)]
    table = lax.all_to_all(spread, ("row", "layer"), 0, 0, tiled=True)
    table = table.reshape(R, L, G, n_idx).transpose(0, 2, 1, 3).reshape(d.N, n_idx)

    inv, cnt, pos, level = pl.pallas_call(
        functools.partial(plan_kernel, d),
        in_specs=[smem, smem, vmem],
        out_specs=[vmem, smem, vmem, smem],
        out_shape=[
            jax.ShapeDtypeStruct((YS, 2, PAIR * NB), I32),
            jax.ShapeDtypeStruct((YS, 2), I32),
            jax.ShapeDtypeStruct((YS, PAIR, NB), I32),
            jax.ShapeDtypeStruct((1,), I32),
        ],
        scratch_shapes=[VMEM((Y, d.N, NB), I32)] * 2,
        compiler_params=limit((2 * Y + 8, d.N, 128), (16, 256, 256)),
        name="plan",
    )(me, table, table)

    most = d.RPD * d.Q * d.S

    def run(branch, me, table, inv, cnt, pos, own, sib, *a_early):
        return body(d.caps[branch], me, table, inv, cnt, pos, own, sib, *a_early)

    def body(caps, me, table, inv, cnt, pos, own, sib, *a_early):
        first, cap = caps
        two = cap > first
        second = max(cap - first, 1)
        e = d.EARLY - 1
        a_late = [
            shift(a_early[e], k - e) if k - e < G - k else shift(a_early[0], k)
            for k in range(d.EARLY, G)
        ]
        packs = pl.pallas_call(
            functools.partial(pack_kernel, d, first, cap),
            in_specs=[smem, smem, smem, hbm, hbm],
            out_specs=[vmem, vmem],
            out_shape=[
                jax.ShapeDtypeStruct((YS, first, T, T), F32),
                jax.ShapeDtypeStruct((YS, second, T, T), F32),
            ],
            scratch_shapes=[pltpu.SemaphoreType.DMA],
            compiler_params=limit((YS, first, T, T), (YS, second, T, T)),
            name="pack",
        )(me, inv, cnt, own, sib)

        def across(piece):
            packed = packs[piece]
            recs = [
                lax.ppermute(
                    packed[k - 1 : k],
                    "row",
                    [(r, ((r // PAIR + k) % Y) * PAIR + r % PAIR) for r in range(R)],
                )
                for k in range(1, Y)
            ]
            rec = recs[0] if len(recs) == 1 else jnp.concatenate(recs, 0)
            return [rec, lax.ppermute(rec, "row", pair_swap)]

        received = [across(0), across(1) if two else [packs[1], packs[1]]]
        a_list = list(a_early) + a_late
        src, aidx, oidx, starts = pl.pallas_call(
            functools.partial(list_kernel, d, first),
            in_specs=[smem, smem, smem],
            out_specs=[smem, smem, smem, smem],
            out_shape=[jax.ShapeDtypeStruct((most,), I32)] * 3
            + [jax.ShapeDtypeStruct((len(d.sections) + 1,), I32)],
            compiler_params=limit(),
            cost_estimate=pl.CostEstimate(flops=5 * 10**9, bytes_accessed=10**5, transcendentals=0),
            name="list",
        )(me, table, pos)

        depth = 8

        def products(k, parts=()):
            _, low, high, part = d.sections[k]
            b_local = [] if part == 1 else [own, sib]
            b_far = received[1 if part == 1 else 0]
            a_part = a_list[low:high]
            size = ((high - low) * d.AR * d.QL, T, T)
            n_a = len(a_part) * d.AR * d.SA
            return pl.pallas_call(
                functools.partial(product_kernel, d, k, depth, first, len(a_part), len(parts)),
                in_specs=[smem] * 5
                + [hbm] * len(b_local)
                + [vmem] * (2 + len(a_part) + len(parts)),
                out_specs=vmem,
                out_shape=jax.ShapeDtypeStruct(size, F32),
                scratch_shapes=[
                    VMEM((n_a, 2 * T, T), BF16),
                    VMEM((depth, T, T), F32),
                    pltpu.SemaphoreType.DMA((depth,)),
                ],
                compiler_params=limit(
                    (depth + 2 * n_a, T, T), size, *(x.shape for x in (*b_far, *parts))
                ),
                cost_estimate=pl.CostEstimate(
                    flops=5 * 10**9, bytes_accessed=10**6, transcendentals=0
                ),
                name="products",
            )(me, src, aidx, oidx, starts, *b_local, *b_far, *a_part, *parts)

        moved = []
        for k, (step, _, _, _) in enumerate(d.sections[:-2]):
            part = products(k)
            moved.append(lax.ppermute(part, "layer", [(l, (l + step) % L) for l in range(L)]))
        mine = products(len(d.sections) - 2)
        return products(len(d.sections) - 1, [mine, *moved])

    result = lax.switch(
        level[0],
        [functools.partial(run, k) for k in range(len(d.caps))],
        me, table, inv, cnt, pos, own, sib, *a_early,
    )
    return result.reshape(d.RPD, 1, d.QL, T, T)


def solution(mesh):
    return jax.shard_map(
        on_device,
        mesh=mesh,
        in_specs=(
            P(("row", "col"), "layer", None, None, None),
            P(("row", "col"), "layer", None),
            P(("row", "col"), "layer", None, None, None),
            P(("row", "col"), "layer", None),
            P("row", "col", None),
        ),
        out_specs=P("row", "col", "layer", None, None),
        check_vma=False,
    )
```
